8 devices in a mesh: dp: 2 (over z, y), sp: 4 (over x, core).
Axes of the slice: x: 2, y: 2, z: 1, core: 2. Of those that a mesh axis runs over, the one named last changes fastest.
Arguments:
- hidden: bfloat16 [256, 2048], P('dp'), parts along dimension 0
- ln_gamma: float32 [2048], replicated
- ln_beta: float32 [2048], replicated
- w_qkv: bfloat16 [2048, 2304], replicated
- w_out: bfloat16 [2048, 2048], replicated
- w_up: bfloat16 [2048, 8192], P(None, 'sp')
- w_down: bfloat16 [8192, 2048], P('sp')
- k_cache: bfloat16 [256, 2048, 128], P('dp', 'sp'), parts along dimension 0
- v_cache: bfloat16 [256, 2048, 128], P('dp', 'sp'), parts along dimension 0
- positions: int32 [256], P('dp'), parts along dimension 0
Outputs:
- output 1: bfloat16 [256, 2048], P('dp'), parts along dimension 0
- output 2: bfloat16 [256, 2048, 128], P('dp', 'sp'), parts along dimension 0
- output 3: bfloat16 [256, 2048, 128], P('dp', 'sp'), parts along dimension 0
There are 2 independent parts. The reference program is written for one: setup_inputs(seed, part) draws one part's arguments, and reference() takes and returns one part's arrays. A program takes and returns all parts, laid end to end along the dimension named above; an argument that names none is the same for every part.
All inputs are finite; a program needn't handle non-finite values.
Results may differ from the reference program's by a relative error of at most 0.00479244.
Values sent between devices are 32-bit elements.
A program may use at most 1 GiB of HBM per device.

```python
import jax
import jax.numpy as jnp
from jax import lax

BATCH_ROWS = 128
D_MODEL = 2048
N_HEADS = 16
HEAD_DIM = 128
FF_DIM = 8192
SEQ_SHARD = 512
N_SHARDS = 4
SEQ_LEN = N_SHARDS * SEQ_SHARD
LN_EPS = 1e-5
ROPE_BASE = 10000.0
NEG_FILL = -1e30


def setup_inputs(seed: int = 0, part: int = 0) -> dict:
    base_key = jax.random.key(seed)
    weight_keys = jax.random.split(base_key, 6)
    part_keys = jax.random.split(jax.random.fold_in(base_key, part), 4)
    hidden = jax.random.normal(part_keys[0], (BATCH_ROWS, D_MODEL), jnp.float32).astype(jnp.bfloat16)
    ln_gamma = 1.0 + 0.3 * jax.random.normal(weight_keys[0], (D_MODEL,), jnp.float32)
    ln_beta = 0.3 * jax.random.normal(weight_keys[1], (D_MODEL,), jnp.float32)
    w_qkv = (jax.random.normal(weight_keys[2], (D_MODEL, (N_HEADS + 2) * HEAD_DIM), jnp.float32) * D_MODEL ** -0.5).astype(jnp.bfloat16)
    out_scale = 0.5 * SEQ_LEN ** 0.5 * (N_HEADS * HEAD_DIM) ** -0.5
    w_out = (jax.random.normal(weight_keys[3], (N_HEADS * HEAD_DIM, D_MODEL), jnp.float32) * out_scale).astype(jnp.bfloat16)
    w_up = (jax.random.normal(weight_keys[4], (D_MODEL, FF_DIM), jnp.float32) * D_MODEL ** -0.5).astype(jnp.bfloat16)
    w_down = (jax.random.normal(weight_keys[5], (FF_DIM, D_MODEL), jnp.float32) * FF_DIM ** -0.5).astype(jnp.bfloat16)
    k_cache = jax.random.normal(part_keys[1], (BATCH_ROWS, SEQ_LEN, HEAD_DIM), jnp.float32).astype(jnp.bfloat16)
    v_cache = jax.random.normal(part_keys[2], (BATCH_ROWS, SEQ_LEN, HEAD_DIM), jnp.float32).astype(jnp.bfloat16)
    positions = jax.random.randint(part_keys[3], (BATCH_ROWS,), SEQ_LEN // 2, SEQ_LEN, dtype=jnp.int32)
    positions = positions.at[0].set(SEQ_LEN - 1).at[1].set(SEQ_LEN // 2)
    return {'hidden': hidden, 'ln_gamma': ln_gamma, 'ln_beta': ln_beta, 'w_qkv': w_qkv, 'w_out': w_out, 'w_up': w_up, 'w_down': w_down, 'k_cache': k_cache, 'v_cache': v_cache, 'positions': positions}


def layer_norm(hidden, ln_gamma, ln_beta):
    hidden_f32 = hidden.astype(jnp.float32)
    row_mean = jnp.mean(hidden_f32, axis=-1, keepdims=True)
    centered = hidden_f32 - row_mean
    row_var = jnp.mean(centered * centered, axis=-1, keepdims=True)
    return (centered * lax.rsqrt(row_var + LN_EPS) * ln_gamma + ln_beta).astype(jnp.bfloat16)


def rotary_tables(positions, head_dim):
    inv_freq = 1.0 / (ROPE_BASE ** (jnp.arange(0, head_dim, 2, dtype=jnp.float32) / head_dim))
    angles = positions.astype(jnp.float32)[:, None] * inv_freq[None, :]
    cos_half = jnp.cos(angles)
    sin_half = jnp.sin(angles)
    return jnp.concatenate([cos_half, cos_half], axis=-1), jnp.concatenate([sin_half, sin_half], axis=-1)


def apply_rotary(vecs, cos_full, sin_full):
    vecs_f32 = vecs.astype(jnp.float32)
    half_dim = vecs.shape[-1] // 2
    rotated = jnp.concatenate([-vecs_f32[..., half_dim:], vecs_f32[..., :half_dim]], axis=-1)
    return (vecs_f32 * cos_full + rotated * sin_full).astype(jnp.bfloat16)


def row_attention(row_inputs):
    q_row, k_row, v_row, pos_row = row_inputs
    scores = jnp.dot(q_row, k_row.T, preferred_element_type=jnp.float32) * HEAD_DIM ** -0.5
    scores = scores.reshape(N_HEADS, N_SHARDS, SEQ_SHARD)
    valid_mask = (jnp.arange(SEQ_LEN) <= pos_row).reshape(N_SHARDS, SEQ_SHARD)
    masked = jnp.where(valid_mask, scores, NEG_FILL)
    block_max = jnp.max(masked, axis=-1)
    exp_scores = jnp.where(valid_mask, jnp.exp(masked - block_max[..., None]), 0.0)
    block_sum = jnp.sum(exp_scores, axis=-1)
    block_ctx = jnp.einsum('hcs,csd->hcd', exp_scores.astype(jnp.bfloat16).astype(jnp.float32), v_row.reshape(N_SHARDS, SEQ_SHARD, HEAD_DIM).astype(jnp.float32))
    top_max = jnp.max(block_max, axis=-1)
    scale_w = jnp.exp(block_max - top_max[:, None])
    total_sum = jnp.sum(block_sum * scale_w, axis=-1)
    total_ctx = jnp.sum(block_ctx * scale_w[..., None], axis=1)
    return (total_ctx / total_sum[:, None]).astype(jnp.bfloat16)


def reference(hidden, ln_gamma, ln_beta, w_qkv, w_out, w_up, w_down, k_cache, v_cache, positions):
    normed = layer_norm(hidden, ln_gamma, ln_beta)
    qkv_proj = jnp.dot(normed, w_qkv, preferred_element_type=jnp.float32).astype(jnp.bfloat16)
    qkv_proj = qkv_proj.reshape(BATCH_ROWS, N_HEADS + 2, HEAD_DIM)
    cos_full, sin_full = rotary_tables(positions, HEAD_DIM)
    q_rot = apply_rotary(qkv_proj[:, :N_HEADS], cos_full[:, None, :], sin_full[:, None, :])
    k_rot = apply_rotary(qkv_proj[:, N_HEADS], cos_full, sin_full)
    v_new = qkv_proj[:, N_HEADS + 1]
    write_mask = (jnp.arange(SEQ_LEN)[None, :] == positions[:, None])[:, :, None]
    k_next = jnp.where(write_mask, k_rot[:, None, :], k_cache)
    v_next = jnp.where(write_mask, v_new[:, None, :], v_cache)
    context = lax.map(row_attention, (q_rot, k_next, v_next, positions))
    attn_out = jnp.dot(context.reshape(BATCH_ROWS, N_HEADS * HEAD_DIM), w_out, preferred_element_type=jnp.float32)
    up_proj = jnp.dot(normed, w_up, preferred_element_type=jnp.float32)
    activated = jax.nn.gelu(up_proj, approximate=False).astype(jnp.bfloat16)
    mlp_out = jnp.dot(activated, w_down, preferred_element_type=jnp.float32)
    out_hidden = (hidden.astype(jnp.float32) + attn_out + mlp_out).astype(jnp.bfloat16)
    return (out_hidden, k_next, v_next)
```

```python
import jax
import jax.numpy as jnp
from jax import lax
from jax.experimental import pallas as pl
from jax.experimental.pallas import tpu as pltpu
from jax.sharding import PartitionSpec as P


MESH = pl.DeviceIdType.MESH
LN_EPS = 1e-5
ROPE_BASE = 10000.0
NEG_FILL = -1e30
HEAD_DIM = 128
BLK = 512
STEP_ROWS = 8
AHEAD = 6
GROUPS = (40, 40, 32, 16)
F32, BF16 = jnp.float32, jnp.bfloat16


def rope_tables(positions):
    inv_freq = 1.0 / (ROPE_BASE ** (jnp.arange(0, HEAD_DIM, 2, dtype=F32) / HEAD_DIM))
    angles = positions.astype(F32)[:, None] * inv_freq[None, :]
    cos_half, sin_half = jnp.cos(angles), jnp.sin(angles)
    return jnp.concatenate([cos_half, cos_half], axis=-1), jnp.concatenate([-sin_half, sin_half], axis=-1)


def layer_kernel(pos_ref, posv_ref, x_hbm, gamma_ref, beta_ref, cos_ref, sin_ref, wqkv_hbm, wup_hbm, wdown_hbm, wout_hbm,
                 k_hbm, v_hbm, kv_ref, mlp_ref, y_ref,
                 xbuf, hbuf, kvw, wbuf, q_s, kn_ref, vn_ref, act, ctx_ref, part, mrecv, arecv, s_loc, s_recv, chip_o, chip_ml, x_o, x_ml,
                 xsem, kvwsem, wsem, osem, ksem, vsem, q_ss, q_rs, m_ss, m_rs, c_ss, c_rs, o_ss, o_rs, t_ss, t_rs, a_ss, a_rs):
    dp, sp = lax.axis_index('dp'), lax.axis_index('sp')
    core = lax.rem(sp, 2)
    mate = (dp, sp + 1 - 2 * core)
    across = (dp, lax.rem(sp + 2, 4))
    rows = xbuf.shape[0]
    n_steps = rows // STEP_ROWS
    seq_dev = k_hbm.shape[1]
    half_heads = q_s.shape[2]
    half_cols = half_heads * HEAD_DIM
    scale = HEAD_DIM ** -0.5

    def weight_copy(src, col, slot, idx):
        return pltpu.make_async_copy(src.at[:, pl.ds(pl.multiple_of(col, BLK), BLK)], wbuf.at[slot], wsem.at[idx])

    def q_copy(j):
        return weight_copy(wqkv_hbm, core * half_cols + j * BLK, j, j)

    def up_copy(j):
        return weight_copy(wup_hbm, j * BLK, 2 + j, 2 + j)

    def down_copy(j):
        half = jnp.where(j < 2, 1 - core, core) if not isinstance(j, int) else ((1 - core) if j < 2 else core)
        return weight_copy(wdown_hbm, half * half_cols + lax.rem(j, 2) * BLK, j, 6 + j)

    def out_copy(j):
        half = (1 - core) if j < 2 else core
        src = wout_hbm.at[pl.ds(pl.multiple_of(core * half_cols, half_cols), half_cols),
                          pl.ds(pl.multiple_of(half * half_cols + (j % 2) * BLK, BLK), BLK)]
        return pltpu.make_async_copy(src, wbuf.at[4 + j // 2, pl.ds((j % 2) * half_cols, half_cols)], osem.at[j])

    def k_copy(i):
        r = pl.ds(i * STEP_ROWS, STEP_ROWS)
        return pltpu.make_async_copy(k_hbm.at[r], kv_ref.at[0, r], ksem.at[i])

    def v_copy(i):
        r = pl.ds(i * STEP_ROWS, STEP_ROWS)
        return pltpu.make_async_copy(v_hbm.at[r], kv_ref.at[1, r], vsem.at[i])

    def cache_start(i):
        k_copy(i).start()
        v_copy(i).start()

    x_copy = pltpu.make_async_copy(x_hbm, xbuf, xsem)
    x_copy.start()
    kvw_copy = pltpu.make_async_copy(wqkv_hbm.at[:, pl.ds(2 * half_cols, 2 * HEAD_DIM)], kvw, kvwsem)
    kvw_copy.start()
    for j in range(2):
        q_copy(j).start()
    for j in range(4):
        up_copy(j).start()

    barrier = pltpu.get_barrier_semaphore()
    for dev in (mate, across):
        pl.semaphore_signal(barrier, inc=1, device_id=dev, device_id_type=MESH)
    pl.semaphore_wait(barrier, 2)

    x_copy.wait()

    def norm_rows(i, _):
        r = pl.ds(pl.multiple_of(i * 16, 16), 16)
        h = xbuf[r, :].astype(F32)
        centered = h - jnp.mean(h, axis=-1, keepdims=True)
        var = jnp.mean(centered * centered, axis=-1, keepdims=True)
        hbuf[r, :] = (centered * lax.rsqrt(var + LN_EPS) * gamma_ref[...] + beta_ref[...]).astype(BF16)
        return 0

    lax.fori_loop(0, rows // 16, norm_rows, 0)

    def rotate(vec):
        vec = vec.astype(BF16).astype(F32)
        return (vec * cos_ref[...] + pltpu.roll(vec, HEAD_DIM // 2, 1) * sin_ref[...]).astype(BF16)

    kvw_copy.wait()
    kv_new = jnp.dot(hbuf[...], kvw[...], preferred_element_type=F32)
    k_new = rotate(kv_new[:, :HEAD_DIM])
    v_new = kv_new[:, HEAD_DIM:].astype(BF16)
    kn_ref[...] = k_new.astype(F32)
    vn_ref[...] = v_new.astype(F32)
    kv_ref[0, rows, 0:rows, :] = k_new
    kv_ref[1, rows, 0:rows, :] = v_new
    at = jnp.broadcast_to(posv_ref[...] - sp * seq_dev, (16, rows))
    tile = lax.shift_right_logical(jnp.clip(at, 0, seq_dev - 1), 4)
    inside = jnp.logical_and(at >= 0, at < seq_dev)
    kv_ref[0, rows, rows:rows + 16, :] = tile.astype(F32).astype(BF16)
    kv_ref[0, rows, rows + 16:rows + 32, :] = jnp.where(inside, at - tile * 16, 16).astype(F32).astype(BF16)

    for j in range(2):
        q_copy(j).wait()
        for n in range(2):
            q_part = jnp.dot(hbuf[...], wbuf[j, :, n * 256:(n + 1) * 256], preferred_element_type=F32)
            for t in range(2):
                q_s[core, :, j * 4 + n * 2 + t, :] = rotate(q_part[:, t * HEAD_DIM:(t + 1) * HEAD_DIM]).astype(F32)
        down_copy(j).start()
    q_send = pltpu.make_async_remote_copy(src_ref=q_s.at[core], dst_ref=q_s.at[core], send_sem=q_ss, recv_sem=q_rs,
                                          device_id=mate, device_id_type=MESH)
    q_send.start()

    def up_step(j, _):
        up_copy(j).wait()
        for n in range(2):
            up = jnp.dot(hbuf[...], wbuf[2 + j, :, n * 256:(n + 1) * 256], preferred_element_type=F32)
            gelu = 0.5 * up * (1.0 + lax.erf(up * (0.5 ** 0.5)))
            act[:, pl.ds(pl.multiple_of(j * BLK + n * 256, 256), 256)] = gelu.astype(BF16)

        @pl.when(j < 2)
        def _():
            down_copy(2 + j).start()

        @pl.when(j >= 2)
        def _():
            cache_start(j - 2)

        return 0

    lax.fori_loop(0, 4, up_step, 0)

    def down_step(j, _):
        down_copy(j).wait()
        for n in range(2):
            part[j // 2, :, pl.ds(pl.multiple_of(lax.rem(j, 2) * BLK + n * 256, 256), 256)] = jnp.dot(
                act[...], wbuf[j, :, n * 256:(n + 1) * 256], preferred_element_type=F32)
        cache_start(2 + j)
        return 0

    m_send = pltpu.make_async_remote_copy(src_ref=part.at[0], dst_ref=mrecv, send_sem=m_ss, recv_sem=m_rs,
                                          device_id=mate, device_id_type=MESH)
    lax.fori_loop(0, 2, down_step, 0)
    m_send.start()
    lax.fori_loop(2, 4, down_step, 0)
    q_send.wait()

    slots = lax.broadcasted_iota(jnp.int32, (2 * half_heads, seq_dev), 1)
    lanes = lax.broadcasted_iota(jnp.int32, (half_heads, 128), 1)
    zero_q = jnp.zeros((2 * half_heads, HEAD_DIM), BF16)

    def attend(i, _):
        k_copy(i).wait()
        v_copy(i).wait()

        @pl.when(i + AHEAD < n_steps)
        def _():
            cache_start(i + AHEAD)

        @pl.when(i == n_steps - AHEAD)
        def _():
            for j in range(4):
                out_copy(j).start()

        for pair in range(STEP_ROWS // 2):
            bs = [i * STEP_ROWS + 2 * pair + t for t in range(2)]
            qf = [jnp.concatenate([q_s[0, b], q_s[1, b]], axis=0) for b in bs]
            qb = [q.astype(BF16) for q in qf]
            lhs = jnp.concatenate([jnp.concatenate([qb[0], zero_q], axis=1), jnp.concatenate([zero_q, qb[1]], axis=1)], axis=0)
            k2 = jnp.concatenate([kv_ref[0, b] for b in bs], axis=1)
            s2 = lax.dot_general(lhs, k2, (((1,), (1,)), ((), ())), preferred_element_type=F32) * scale
            probs, stats = [], []
            for t, b in enumerate(bs):
                at = pos_ref[b] - sp * seq_dev
                s = s2[t * 2 * half_heads:(t + 1) * 2 * half_heads]
                old = slots < at
                here = jnp.logical_and(at >= 0, at < seq_dev)
                masked = jnp.where(old, s, NEG_FILL)
                s_new = jnp.sum(qf[t] * kn_ref[pl.ds(b, 1), :], axis=-1, keepdims=True) * scale
                s_new = jnp.where(here, s_new, NEG_FILL)
                m = jnp.maximum(jnp.max(masked, axis=-1, keepdims=True), s_new)
                e = jnp.where(old, jnp.exp(masked - m), 0.0)
                e_new = jnp.where(here, jnp.exp(s_new - m), 0.0)
                l = jnp.sum(e, axis=-1, keepdims=True) + e_new
                probs.append(e.astype(BF16))
                stats.append((m, l, e_new.astype(BF16).astype(F32) * vn_ref[pl.ds(b, 1), :]))
            v2 = jnp.concatenate([kv_ref[1, b] for b in bs], axis=1)
            o2 = jnp.dot(jnp.concatenate(probs, axis=0), v2, preferred_element_type=F32)
            for t, b in enumerate(bs):
                m, l, extra = stats[t]
                o = o2[t * 2 * half_heads:(t + 1) * 2 * half_heads, t * HEAD_DIM:(t + 1) * HEAD_DIM] + extra
                mb = jnp.broadcast_to(m, o.shape)
                lb = jnp.broadcast_to(l, o.shape)
                for f in range(2):
                    hs = slice(f * half_heads, (f + 1) * half_heads)
                    s_loc[f, b, 0] = o[hs]
                    s_loc[f, b, 1] = mb[hs]
                    s_loc[f, b, 2] = lb[hs]
        return 0

    starts = [sum(GROUPS[:g]) for g in range(len(GROUPS))]

    def swap_copy(g):
        r = pl.ds(starts[g], GROUPS[g])
        return pltpu.make_async_remote_copy(src_ref=s_loc.at[1 - core, r], dst_ref=s_recv.at[r], send_sem=c_ss.at[g],
                                            recv_sem=c_rs.at[g], device_id=mate, device_id_type=MESH)

    def cross_copies(g):
        r = pl.ds(starts[g], GROUPS[g])
        return (pltpu.make_async_remote_copy(src_ref=chip_o.at[r], dst_ref=x_o.at[r], send_sem=o_ss.at[g],
                                             recv_sem=o_rs.at[g], device_id=across, device_id_type=MESH),
                pltpu.make_async_remote_copy(src_ref=chip_ml.at[g], dst_ref=x_ml.at[g], send_sem=t_ss.at[g],
                                             recv_sem=t_rs.at[g], device_id=across, device_id_type=MESH))

    def merge_chip(g):
        swap_copy(g).wait()

        def body(i, tiles):
            tm, tl = tiles
            for u in range(8):
                b = starts[g] + i * 8 + u
                m_a, m_b = s_loc[core, b, 1], s_recv[b, 1]
                top = jnp.maximum(m_a, m_b)
                w_a, w_b = jnp.exp(m_a - top), jnp.exp(m_b - top)
                chip_o[b] = s_loc[core, b, 0] * w_a + s_recv[b, 0] * w_b
                total = s_loc[core, b, 2] * w_a + s_recv[b, 2] * w_b
                s_recv[b, 1] = top
                s_recv[b, 2] = total
                hit = lanes == i * 8 + u
                tm = jnp.where(hit, top, tm)
                tl = jnp.where(hit, total, tl)
            return tm, tl

        zero = jnp.zeros((half_heads, 128), F32)
        tm, tl = lax.fori_loop(0, GROUPS[g] // 8, body, (zero, zero))
        chip_ml[g, 0] = tm
        chip_ml[g, 1] = tl
        for copy in cross_copies(g):
            copy.start()

    def merge_all(g):
        for copy in cross_copies(g):
            copy.wait()
        tm, tl = x_ml[g, 0], x_ml[g, 1]

        def body(i, _):
            for u in range(8):
                b = starts[g] + i * 8 + u
                hit = lanes == i * 8 + u
                m_b = jnp.sum(jnp.where(hit, tm, 0.0), axis=-1, keepdims=True)
                l_b = jnp.sum(jnp.where(hit, tl, 0.0), axis=-1, keepdims=True)
                m_a = s_recv[b, 1]
                top = jnp.maximum(m_a, m_b)
                w_a, w_b = jnp.exp(m_a - top), jnp.exp(m_b - top)
                total = s_recv[b, 2] * w_a + l_b * w_b
                x_o[b] = (chip_o[b] * w_a + x_o[b] * w_b) / total
            return 0

        lax.fori_loop(0, GROUPS[g] // 8, body, 0)

    n_groups = len(GROUPS)
    for g in range(n_groups):
        lax.fori_loop(starts[g] // STEP_ROWS, (starts[g] + GROUPS[g]) // STEP_ROWS, attend, 0)
        swap_copy(g).start()
        if g == 0:
            m_send.wait()
            mlp_ref[...] = part[1] + mrecv[...]
        if g >= 1:
            merge_chip(g - 1)
        if g >= 2:
            merge_all(g - 2)
    merge_chip(n_groups - 1)
    merge_all(n_groups - 2)
    merge_all(n_groups - 1)
    for h in range(half_heads):
        ctx_ref[:, h * HEAD_DIM:(h + 1) * HEAD_DIM] = x_o[:, h, :].astype(BF16)

    def attn_copy(j):
        c = slice(j * BLK, (j + 1) * BLK)
        return pltpu.make_async_remote_copy(src_ref=part.at[0, :, c], dst_ref=arecv.at[:, c], send_sem=a_ss.at[j],
                                            recv_sem=a_rs.at[j], device_id=mate, device_id_type=MESH)

    for j in range(4):
        out_copy(j).wait()
        for n in range(2):
            c = slice((j % 2) * BLK + n * 256, (j % 2) * BLK + (n + 1) * 256)
            part[j // 2, :, c] = jnp.dot(ctx_ref[...], wbuf[4 + j // 2, (j % 2) * half_cols:(j % 2 + 1) * half_cols, n * 256:(n + 1) * 256],
                                         preferred_element_type=F32)
        if j < 2:
            attn_copy(j).start()
    for j in range(2):
        c = slice(j * BLK, (j + 1) * BLK)
        attn_copy(j).wait()
        y_ref[:, c] = part[1, :, c] + arecv[:, c]


def store_kernel(kv_ref, k_out, v_out, fresh, tiles, idx_v, idx_s, kvsem, tsem, isem):
    rows = k_out.shape[0]
    n_parts = kvsem.shape[1]
    per = rows // n_parts
    outs = (k_out, v_out)

    def big(a, p):
        r = pl.ds(p * per, per)
        return pltpu.make_async_copy(kv_ref.at[a, r], outs[a].at[r], kvsem.at[a, p])

    for a in range(2):
        for p in range(n_parts):
            big(a, p).start()

    idx_v[...] = kv_ref[0, rows, rows:rows + 32, :].astype(F32).astype(jnp.int32)
    idx_copy = pltpu.make_async_copy(idx_v, idx_s, isem)
    idx_copy.start()
    for a in range(2):
        fresh[a] = kv_ref[a, rows, 0:rows, :].astype(F32)
    idx_copy.wait()

    def tile_start(b):
        return pl.multiple_of(idx_s[0, b] * 16, 16)

    ids = lax.broadcasted_iota(jnp.int32, (16, HEAD_DIM), 0)

    def make_tile(b, _):
        hit = ids == idx_s[16, b]
        for a in range(2):
            old = kv_ref[a, b, pl.ds(tile_start(b), 16), :].astype(F32)
            tiles[a, b] = jnp.where(hit, fresh[a, pl.ds(b, 1), :], old).astype(BF16)
        return 0

    lax.fori_loop(0, rows, make_tile, 0, unroll=4)

    def small(a, b):
        return pltpu.make_async_copy(tiles.at[a, b], outs[a].at[b, pl.ds(tile_start(b), 16)], tsem.at[a, b])

    for a in range(2):
        for p in range(n_parts):
            big(a, p).wait()

            def put(b, _):
                small(a, b).start()
                return 0

            lax.fori_loop(p * per, (p + 1) * per, put, 0)
    for a in range(2):
        def done(b, _):
            small(a, b).wait()
            return 0

        lax.fori_loop(0, rows, done, 0)


ANY = pl.BlockSpec(memory_space=pl.ANY)
VM = pl.BlockSpec(memory_space=pltpu.VMEM)
SM = pl.BlockSpec(memory_space=pltpu.SMEM)
HB = pl.BlockSpec(memory_space=pltpu.HBM)


def device_step(hidden, ln_gamma, ln_beta, w_qkv, w_out, w_up, w_down, k_cache, v_cache, positions):
    rows, d_model = hidden.shape
    half_heads = w_out.shape[0] // HEAD_DIM // 2
    half_cols = half_heads * HEAD_DIM
    n_steps, n_groups = rows // STEP_ROWS, len(GROUPS)
    cos_full, sin_full = rope_tables(positions)
    dma = pltpu.SemaphoreType.DMA
    kv, mlp_chip, y = pl.pallas_call(
        layer_kernel,
        in_specs=[SM, VM, HB, VM, VM, VM, VM, HB, HB, HB, HB, HB, HB],
        out_specs=[VM] * 3,
        out_shape=[pltpu.VMEM((2, rows + 1) + k_cache.shape[1:], BF16),
                   jax.ShapeDtypeStruct((rows, half_cols), F32),
                   jax.ShapeDtypeStruct((rows, half_cols), F32)],
        scratch_shapes=[
            pltpu.VMEM((rows, d_model), BF16), pltpu.VMEM((rows, d_model), BF16),
            pltpu.VMEM((d_model, 2 * HEAD_DIM), BF16), pltpu.VMEM((6, d_model, BLK), BF16),
            pltpu.VMEM((2, rows, half_heads, HEAD_DIM), F32),
            pltpu.VMEM((rows, HEAD_DIM), F32), pltpu.VMEM((rows, HEAD_DIM), F32),
            pltpu.VMEM((rows, w_up.shape[1]), BF16), pltpu.VMEM((rows, half_cols), BF16),
            pltpu.VMEM((2, rows, half_cols), F32), pltpu.VMEM((rows, half_cols), F32), pltpu.VMEM((rows, half_cols), F32),
            pltpu.VMEM((2, rows, 3, half_heads, HEAD_DIM), F32),
            pltpu.VMEM((rows, 3, half_heads, HEAD_DIM), F32),
            pltpu.VMEM((rows, half_heads, HEAD_DIM), F32), pltpu.VMEM((n_groups, 2, half_heads, 128), F32),
            pltpu.VMEM((rows, half_heads, HEAD_DIM), F32), pltpu.VMEM((n_groups, 2, half_heads, 128), F32),
            dma, dma, dma((10,)), dma((4,)), dma((n_steps,)), dma((n_steps,)), dma, dma, dma, dma,
            dma((n_groups,)), dma((n_groups,)), dma((n_groups,)), dma((n_groups,)), dma((n_groups,)), dma((n_groups,)),
            dma((2,)), dma((2,)),
        ],
        compiler_params=pltpu.CompilerParams(collective_id=0, has_side_effects=True, vmem_limit_bytes=27 << 20),
    )(positions, positions.reshape(1, -1), hidden, ln_gamma.reshape(1, -1), ln_beta.reshape(1, -1), cos_full, sin_full,
      w_qkv, w_up, w_down, w_out, k_cache, v_cache)

    mlp_far = lax.ppermute(mlp_chip, 'sp', [(0, 2), (2, 0), (1, 3), (3, 1)])

    k_next, v_next = pl.pallas_call(
        store_kernel,
        in_specs=[VM],
        out_specs=[HB, HB],
        out_shape=[jax.ShapeDtypeStruct(k_cache.shape, BF16), jax.ShapeDtypeStruct(k_cache.shape, BF16)],
        scratch_shapes=[pltpu.VMEM((2, rows, HEAD_DIM), F32), pltpu.VMEM((2, rows, 16, HEAD_DIM), BF16),
                        pltpu.VMEM((32, rows), jnp.int32), pltpu.SMEM((32, rows), jnp.int32),
                        dma((2, 4)), dma((2, rows)), dma],
        compiler_params=pltpu.CompilerParams(vmem_limit_bytes=4 << 20),
        cost_estimate=pl.CostEstimate(flops=40_000_000_000, bytes_accessed=32 << 20, transcendentals=0),
    )(kv)

    half = y + (mlp_chip + mlp_far)
    mate_half = lax.ppermute(half, 'sp', [(0, 1), (1, 0), (2, 3), (3, 2)])
    first = (lax.axis_index('sp') % 2) == 0
    branches = jnp.concatenate([jnp.where(first, half, mate_half), jnp.where(first, mate_half, half)], axis=-1)
    out_hidden = (hidden.astype(F32) + branches).astype(BF16)
    return out_hidden, k_next, v_next


def solution(mesh):
    cache_spec = P('dp', 'sp', None)
    in_specs = (P('dp', None), P(None), P(None), P(None, None), P(None, None), P(None, 'sp'), P('sp', None), cache_spec, cache_spec, P('dp'))
    out_specs = (P('dp', None), cache_spec, cache_spec)
    return jax.shard_map(device_step, mesh=mesh, in_specs=in_specs, out_specs=out_specs, check_vma=False)
```

```python
import jax
import jax.numpy as jnp
import numpy as np
from jax import lax
from jax.experimental import pallas as pl
from jax.experimental.pallas import tpu as pltpu
from jax.sharding import PartitionSpec as P


MESH = pl.DeviceIdType.MESH
LN_EPS = 1e-5
ROPE_BASE = 10000.0
NEG_FILL = -1e30
HEAD_DIM = 128
BLK = 512
STEP_ROWS = 8
SLOTS = 7
FAR_GROUPS = (32, 32)
OWN_GROUPS = (32, 24, 8)
F32, BF16 = jnp.float32, jnp.bfloat16


def rope_tables(positions):
    inv_freq = (ROPE_BASE ** (-np.arange(0, HEAD_DIM, 2) / HEAD_DIM)).astype(np.float32)
    angles = positions.astype(F32)[:, None] * inv_freq[None, :]
    cos_half, sin_half = jnp.cos(angles), jnp.sin(angles)
    return jnp.concatenate([cos_half, cos_half], axis=-1), jnp.concatenate([-sin_half, sin_half], axis=-1)


def layer_kernel(pos_hbm, posv_hbm, x_hbm, gamma_hbm, beta_hbm, cos_hbm, sin_hbm, wqkv_hbm, wup_hbm, wdown_hbm, wout_hbm,
                 k_hbm, v_hbm, kv_ref, z_ref,
                 pos_ref, posv_ref, gamma_ref, beta_ref, cos_ref, sin_ref,
                 xbuf, hbuf, kvw, wbuf, q_s, kn_ref, vn_ref, act, ctx_ref, part, mrecv, mx_recv, mlp_own, mlp_mate, arecv,
                 s_loc, s_recv, chip_o, chip_ml, x_o, x_ml,
                 insem, xsem, kvwsem, wsem, osem, ksem, vsem, q_ss, q_rs, m_ss, m_rs, mx_ss, mx_rs, mm_ss, mm_rs,
                 c_ss, c_rs, o_ss, o_rs, t_ss, t_rs, a_ss, a_rs):
    dp, sp = lax.axis_index('dp'), lax.axis_index('sp')
    core = lax.rem(sp, 2)
    chip = lax.div(sp, 2)
    mate = (dp, sp + 1 - 2 * core)
    across = (dp, lax.rem(sp + 2, 4))
    rows = xbuf.shape[0]
    own_rows = rows // 2
    n_steps = rows // STEP_ROWS
    seq_dev = k_hbm.shape[1]
    half_heads = q_s.shape[2]
    half_cols = half_heads * HEAD_DIM
    scale = HEAD_DIM ** -0.5
    own_base = pl.multiple_of(chip * own_rows, own_rows)
    far_base = pl.multiple_of((1 - chip) * own_rows, own_rows)

    def weight_copy(src, col, slot, idx):
        return pltpu.make_async_copy(src.at[:, pl.ds(pl.multiple_of(col, BLK), BLK)], wbuf.at[slot], wsem.at[idx])

    def q_copy(j):
        return weight_copy(wqkv_hbm, core * half_cols + j * BLK, j, j)

    def up_copy(j):
        return weight_copy(wup_hbm, j * BLK, 2 + j, 2 + j)

    def down_copy(j):
        half = jnp.where(j < 2, 1 - core, core)
        return weight_copy(wdown_hbm, half * half_cols + lax.rem(j, 2) * BLK, lax.rem(6 + j, SLOTS), 6 + j)

    def out_copy(j):
        half = (1 - core) if j < 2 else core
        src = wout_hbm.at[pl.ds(pl.multiple_of(core * half_cols, half_cols), half_cols),
                          pl.ds(pl.multiple_of(half * half_cols + (j % 2) * BLK, BLK), BLK)]
        return pltpu.make_async_copy(src, wbuf.at[3 + j // 2, pl.ds((j % 2) * half_cols, half_cols)], osem.at[j])

    def first_row(i):
        return pl.multiple_of(lax.rem((1 - chip) * own_rows + i * STEP_ROWS, rows), STEP_ROWS)

    def k_copy(i):
        r = pl.ds(first_row(i), STEP_ROWS)
        return pltpu.make_async_copy(k_hbm.at[r], kv_ref.at[0, r], ksem.at[i])

    def v_copy(i):
        r = pl.ds(first_row(i), STEP_ROWS)
        return pltpu.make_async_copy(v_hbm.at[r], kv_ref.at[1, r], vsem.at[i])

    def cache_start(i):
        k_copy(i).start()
        v_copy(i).start()

    x_copy = pltpu.make_async_copy(x_hbm, xbuf, xsem)
    x_copy.start()
    small = [pltpu.make_async_copy(src, dst, insem.at[n]) for n, (src, dst) in enumerate((
        (gamma_hbm, gamma_ref), (beta_hbm, beta_ref), (cos_hbm, cos_ref), (sin_hbm, sin_ref), (posv_hbm, posv_ref),
        (pos_hbm, pos_ref)))]
    for copy in small:
        copy.start()
    kvw_copy = pltpu.make_async_copy(wqkv_hbm.at[:, pl.ds(2 * half_cols, 2 * HEAD_DIM)], kvw, kvwsem)
    kvw_copy.start()
    for j in range(2):
        q_copy(j).start()
    for j in range(4):
        up_copy(j).start()
    down_copy(0).start()

    barrier = pltpu.get_barrier_semaphore()
    for dev in (mate, across):
        pl.semaphore_signal(barrier, inc=1, device_id=dev, device_id_type=MESH)
    pl.semaphore_wait(barrier, 2)

    x_copy.wait()
    for copy in small:
        copy.wait()

    def norm_rows(i, _):
        for u in range(2):
            r = pl.ds(pl.multiple_of(i * 32 + u * 16, 16), 16)
            h = xbuf[r, :].astype(F32)
            centered = h - jnp.mean(h, axis=-1, keepdims=True)
            var = jnp.mean(centered * centered, axis=-1, keepdims=True)
            hbuf[r, :] = (centered * lax.rsqrt(var + LN_EPS) * gamma_ref[...] + beta_ref[...]).astype(BF16)
        return 0

    lax.fori_loop(0, rows // 32, norm_rows, 0)

    def rotate(vec):
        vec = vec.astype(BF16).astype(F32)
        return (vec * cos_ref[...] + pltpu.roll(vec, HEAD_DIM // 2, 1) * sin_ref[...]).astype(BF16)

    kvw_copy.wait()
    kv_new = jnp.dot(hbuf[...], kvw[...], preferred_element_type=F32)
    k_new = rotate(kv_new[:, :HEAD_DIM])
    v_new = kv_new[:, HEAD_DIM:].astype(BF16)
    kn_ref[...] = k_new.astype(F32)
    vn_ref[...] = v_new.astype(F32)
    kv_ref[0, rows, 0:rows, :] = k_new
    kv_ref[1, rows, 0:rows, :] = v_new
    at = jnp.broadcast_to(posv_ref[...] - sp * seq_dev, (16, rows))
    tile = lax.shift_right_logical(jnp.clip(at, 0, seq_dev - 1), 4)
    inside = jnp.logical_and(at >= 0, at < seq_dev)
    kv_ref[0, rows, rows:rows + 16, :] = tile.astype(F32).astype(BF16)
    kv_ref[0, rows, rows + 16:rows + 32, :] = jnp.where(inside, at - tile * 16, 16).astype(F32).astype(BF16)

    for j in range(2):
        q_copy(j).wait()
        for n in range(2):
            q_part = jnp.dot(hbuf[...], wbuf[j, :, n * 256:(n + 1) * 256], preferred_element_type=F32)
            for t in range(2):
                q_s[core, :, j * 4 + n * 2 + t, :] = rotate(q_part[:, t * HEAD_DIM:(t + 1) * HEAD_DIM]).astype(F32)
        down_copy(1 + j).start()
    q_send = pltpu.make_async_remote_copy(src_ref=q_s.at[core], dst_ref=q_s.at[core], send_sem=q_ss, recv_sem=q_rs,
                                          device_id=mate, device_id_type=MESH)
    q_send.start()

    def up_step(j, _):
        up_copy(j).wait()
        for n in range(2):
            up = jnp.dot(hbuf[...], wbuf[2 + j, :, n * 256:(n + 1) * 256], preferred_element_type=F32)
            gelu = 0.5 * up * (1.0 + lax.erf(up * (0.5 ** 0.5)))
            act[:, pl.ds(pl.multiple_of(j * BLK + n * 256, 256), 256)] = gelu.astype(BF16)

        @pl.when(j == 0)
        def _():
            down_copy(3).start()
            cache_start(0)

        @pl.when(j > 0)
        def _():
            cache_start(2 * j - 1)
            cache_start(2 * j)

        return 0

    lax.fori_loop(0, 4, up_step, 0)

    def down_step(j, _):
        down_copy(j).wait()
        slot = lax.rem(6 + j, SLOTS)
        for n in range(2):
            part[j // 2, :, pl.ds(pl.multiple_of(lax.rem(j, 2) * BLK + n * 256, 256), 256)] = jnp.dot(
                act[...], wbuf[slot, :, n * 256:(n + 1) * 256], preferred_element_type=F32)
        cache_start(7 + 2 * j)
        cache_start(8 + 2 * j)
        return 0

    m_send = pltpu.make_async_remote_copy(src_ref=part.at[0], dst_ref=mrecv, send_sem=m_ss, recv_sem=m_rs,
                                          device_id=mate, device_id_type=MESH)
    lax.fori_loop(0, 2, down_step, 0)
    m_send.start()
    lax.fori_loop(2, 4, down_step, 0)
    cache_start(n_steps - 1)
    for j in range(4):
        out_copy(j).start()
    m_send.wait()
    part[1] = part[1] + mrecv[...]
    mx_send = pltpu.make_async_remote_copy(src_ref=part.at[1, pl.ds(far_base, own_rows)], dst_ref=mx_recv, send_sem=mx_ss,
                                           recv_sem=mx_rs, device_id=across, device_id_type=MESH)
    mx_send.start()
    q_send.wait()

    slots = lax.broadcasted_iota(jnp.int32, (2 * half_heads, seq_dev), 1)
    lanes = lax.broadcasted_iota(jnp.int32, (half_heads, 128), 1)
    zero_q = jnp.zeros((2 * half_heads, HEAD_DIM), BF16)

    def attend(i, _):
        k_copy(i).wait()
        v_copy(i).wait()
        row = first_row(i)
        for pair in range(STEP_ROWS // 2):
            bs = [row + 2 * pair + t for t in range(2)]
            qf = [jnp.concatenate([q_s[0, b], q_s[1, b]], axis=0) for b in bs]
            qb = [q.astype(BF16) for q in qf]
            lhs = jnp.concatenate([jnp.concatenate([qb[0], zero_q], axis=1), jnp.concatenate([zero_q, qb[1]], axis=1)], axis=0)
            k2 = jnp.concatenate([kv_ref[0, b] for b in bs], axis=1)
            s2 = lax.dot_general(lhs, k2, (((1,), (1,)), ((), ())), preferred_element_type=F32) * scale
            probs, stats = [], []
            for t, b in enumerate(bs):
                at = pos_ref[b] - sp * seq_dev
                s = s2[t * 2 * half_heads:(t + 1) * 2 * half_heads]
                old = slots < at
                here = jnp.logical_and(at >= 0, at < seq_dev)
                masked = jnp.where(old, s, NEG_FILL)
                s_new = jnp.sum(qf[t] * kn_ref[pl.ds(b, 1), :], axis=-1, keepdims=True) * scale
                s_new = jnp.where(here, s_new, NEG_FILL)
                m = jnp.maximum(jnp.max(masked, axis=-1, keepdims=True), s_new)
                e = jnp.where(old, jnp.exp(masked - m), 0.0)
                e_new = jnp.where(here, jnp.exp(s_new - m), 0.0)
                l = jnp.sum(e, axis=-1, keepdims=True) + e_new
                probs.append(e.astype(BF16))
                stats.append((m, l, e_new.astype(BF16).astype(F32) * vn_ref[pl.ds(b, 1), :]))
            v2 = jnp.concatenate([kv_ref[1, b] for b in bs], axis=1)
            o2 = jnp.dot(jnp.concatenate(probs, axis=0), v2, preferred_element_type=F32)
            for t in range(2):
                m, l, extra = stats[t]
                o = o2[t * 2 * half_heads:(t + 1) * 2 * half_heads, t * HEAD_DIM:(t + 1) * HEAD_DIM] + extra
                mb = jnp.broadcast_to(m, o.shape)
                lb = jnp.broadcast_to(l, o.shape)
                turn = i * STEP_ROWS + 2 * pair + t
                for f in range(2):
                    hs = slice(f * half_heads, (f + 1) * half_heads)
                    s_loc[f, turn, 0] = o[hs]
                    s_loc[f, turn, 1] = mb[hs]
                    s_loc[f, turn, 2] = lb[hs]
        return 0

    sizes = FAR_GROUPS + OWN_GROUPS
    starts = [sum(sizes[:g]) for g in range(len(sizes))]
    n_far = len(FAR_GROUPS)

    def swap_copy(g):
        r = pl.ds(starts[g], sizes[g])
        return pltpu.make_async_remote_copy(src_ref=s_loc.at[1 - core, r], dst_ref=s_recv.at[r], send_sem=c_ss.at[g],
                                            recv_sem=c_rs.at[g], device_id=mate, device_id_type=MESH)

    def cross_copies(g):
        r = pl.ds(starts[g], sizes[g])
        return (pltpu.make_async_remote_copy(src_ref=chip_o.at[r], dst_ref=x_o.at[r], send_sem=o_ss.at[g],
                                             recv_sem=o_rs.at[g], device_id=across, device_id_type=MESH),
                pltpu.make_async_remote_copy(src_ref=chip_ml.at[g], dst_ref=x_ml.at[g], send_sem=t_ss.at[g],
                                             recv_sem=t_rs.at[g], device_id=across, device_id_type=MESH))

    def merge_far(g):
        swap_copy(g).wait()

        def body(i, tiles):
            tm, tl = tiles
            for u in range(8):
                b = starts[g] + i * 8 + u
                m_a, m_b = s_loc[core, b, 1], s_recv[b, 1]
                top = jnp.maximum(m_a, m_b)
                w_a, w_b = jnp.exp(m_a - top), jnp.exp(m_b - top)
                chip_o[b] = s_loc[core, b, 0] * w_a + s_recv[b, 0] * w_b
                total = s_loc[core, b, 2] * w_a + s_recv[b, 2] * w_b
                hit = lanes == i * 8 + u
                tm = jnp.where(hit, top, tm)
                tl = jnp.where(hit, total, tl)
            return tm, tl

        zero = jnp.zeros((half_heads, 128), F32)
        tm, tl = lax.fori_loop(0, sizes[g] // 8, body, (zero, zero))
        chip_ml[g, 0] = tm
        chip_ml[g, 1] = tl
        for copy in cross_copies(g):
            copy.start()

    def merge_own(g):
        swap_copy(g).wait()

        def body(i, _):
            for u in range(8):
                b = starts[g] + i * 8 + u
                src = b - own_rows
                part_g = starts[g] - own_rows
                xg = [n for n in range(n_far) if starts[n] <= part_g][-1]
                hit = lanes == src - starts[xg]
                m_x = jnp.sum(jnp.where(hit, x_ml[xg, 0], 0.0), axis=-1, keepdims=True)
                l_x = jnp.sum(jnp.where(hit, x_ml[xg, 1], 0.0), axis=-1, keepdims=True)
                m_a, m_b = s_loc[core, b, 1], s_recv[b, 1]
                top = jnp.maximum(jnp.maximum(m_a, m_b), m_x)
                w_a, w_b, w_x = jnp.exp(m_a - top), jnp.exp(m_b - top), jnp.exp(m_x - top)
                total = s_loc[core, b, 2] * w_a + s_recv[b, 2] * w_b + l_x * w_x
                x_o[src] = (s_loc[core, b, 0] * w_a + s_recv[b, 0] * w_b + x_o[src] * w_x) / total
            return 0

        lax.fori_loop(0, sizes[g] // 8, body, 0)

    def run_group(g):
        lax.fori_loop(starts[g] // STEP_ROWS, (starts[g] + sizes[g]) // STEP_ROWS, attend, 0)
        swap_copy(g).start()

    def cross_wait(g):
        for copy in cross_copies(g):
            copy.wait()

    mm_send = pltpu.make_async_remote_copy(src_ref=mlp_own, dst_ref=mlp_mate, send_sem=mm_ss, recv_sem=mm_rs,
                                           device_id=mate, device_id_type=MESH)
    run_group(0)
    run_group(1)
    merge_far(0)
    run_group(2)
    merge_far(1)
    run_group(3)
    mx_send.wait()
    mlp_own[...] = part[1, pl.ds(own_base, own_rows), :] + mx_recv[...]
    mm_send.start()
    run_group(4)
    cross_wait(0)
    merge_own(2)
    cross_wait(1)
    merge_own(3)
    merge_own(4)
    for h in range(half_heads):
        ctx_ref[:, h * HEAD_DIM:(h + 1) * HEAD_DIM] = x_o[:, h, :].astype(BF16)
    mm_send.wait()

    def attn_copy(j):
        return pltpu.make_async_remote_copy(src_ref=part.at[0, pl.ds(j % 2 * own_rows, own_rows), pl.ds(j // 2 * BLK, BLK)],
                                            dst_ref=arecv.at[j], send_sem=a_ss.at[j], recv_sem=a_rs.at[j],
                                            device_id=mate, device_id_type=MESH)

    def block(j):
        return part.at[0, pl.ds(j % 2 * own_rows, own_rows), pl.ds(j // 2 * BLK, BLK)]

    for j in range(4):
        out_copy(j).wait()
        for n in range(2):
            block(j)[:, n * 256:(n + 1) * 256] = jnp.dot(
                ctx_ref[...], wbuf[3 + j // 2, (j % 2) * half_cols:(j % 2 + 1) * half_cols, n * 256:(n + 1) * 256],
                preferred_element_type=F32)
        attn_copy(j).start()
    for j in range(4):
        attn_copy(j).wait()
    for j in range(4):
        half = (1 - core) if j < 2 else core
        mlp = mlp_mate if j < 2 else mlp_own
        col = pl.multiple_of(half * half_cols + (j % 2) * BLK, BLK)
        z_ref[:, pl.ds(col, BLK)] = block(j)[...] + arecv[(j + 2) % 4] + mlp[:, (j % 2) * BLK:(j % 2 + 1) * BLK]


def store_kernel(kv_ref, k_out, v_out, fresh, tiles, idx_v, idx_s, kvsem, tsem, isem):
    rows = k_out.shape[0]
    n_parts = kvsem.shape[1]
    per = rows // n_parts
    outs = (k_out, v_out)

    def big(a, p):
        r = pl.ds(p * per, per)
        return pltpu.make_async_copy(kv_ref.at[a, r], outs[a].at[r], kvsem.at[a, p])

    idx_v[...] = kv_ref[0, rows, rows:rows + 32, :].astype(F32).astype(jnp.int32)
    idx_copy = pltpu.make_async_copy(idx_v, idx_s, isem)
    idx_copy.start()
    for p in range(n_parts):
        for a in range(2):
            big(a, p).start()
    for a in range(2):
        fresh[a] = kv_ref[a, rows, 0:rows, :].astype(F32)
    idx_copy.wait()
    ids = lax.broadcasted_iota(jnp.int32, (16, HEAD_DIM), 0)

    def tile_of(b):
        return pl.ds(pl.multiple_of(idx_s[0, b] * 16, 16), 16)

    def make_tile(b, _):
        hit = ids == idx_s[16, b]
        for a in range(2):
            old = kv_ref[a, b, tile_of(b), :].astype(F32)
            tiles[a, b] = jnp.where(hit, fresh[a, pl.ds(b, 1), :], old).astype(BF16)
        return 0

    lax.fori_loop(0, rows, make_tile, 0, unroll=8)

    for p in range(n_parts):
        for a in range(2):
            big(a, p).wait()

        def put(b, _):
            for a in range(2):
                pltpu.make_async_copy(tiles.at[a, b], outs[a].at[b, tile_of(b)], tsem.at[a]).start()
            return 0

        lax.fori_loop(p * per, (p + 1) * per, put, 0, unroll=4)
    for a in range(2):
        pltpu.make_async_copy(tiles.at[a], outs[a].at[:, pl.ds(0, 16)], tsem.at[a]).wait()


ANY = pl.BlockSpec(memory_space=pl.ANY)
VM = pl.BlockSpec(memory_space=pltpu.VMEM)
SM = pl.BlockSpec(memory_space=pltpu.SMEM)
HB = pl.BlockSpec(memory_space=pltpu.HBM)


def device_step(hidden, ln_gamma, ln_beta, w_qkv, w_out, w_up, w_down, k_cache, v_cache, positions):
    rows, d_model = hidden.shape
    half_heads = w_out.shape[0] // HEAD_DIM // 2
    half_cols = half_heads * HEAD_DIM
    own_rows = rows // 2
    n_steps, n_far, n_all = rows // STEP_ROWS, len(FAR_GROUPS), len(FAR_GROUPS) + len(OWN_GROUPS)
    positions, upper = lax.optimization_barrier((positions, lax.axis_index('sp') < 2))
    cos_full, sin_full = rope_tables(positions)
    dma = pltpu.SemaphoreType.DMA
    heads_f32 = (half_heads, HEAD_DIM)
    kv, z = pl.pallas_call(
        layer_kernel,
        in_specs=[HB] * 13,
        out_specs=[VM] * 2,
        out_shape=[pltpu.VMEM((2, rows + 1) + k_cache.shape[1:], BF16), jax.ShapeDtypeStruct((own_rows, d_model), F32)],
        scratch_shapes=[
            pltpu.SMEM((rows,), jnp.int32), pltpu.VMEM((1, rows), jnp.int32),
            pltpu.VMEM((1, d_model), F32), pltpu.VMEM((1, d_model), F32),
            pltpu.VMEM((rows, HEAD_DIM), F32), pltpu.VMEM((rows, HEAD_DIM), F32),
            pltpu.VMEM((rows, d_model), BF16), pltpu.VMEM((rows, d_model), BF16),
            pltpu.VMEM((d_model, 2 * HEAD_DIM), BF16), pltpu.VMEM((SLOTS, d_model, BLK), BF16),
            pltpu.VMEM((2, rows) + heads_f32, F32),
            pltpu.VMEM((rows, HEAD_DIM), F32), pltpu.VMEM((rows, HEAD_DIM), F32),
            pltpu.VMEM((rows, w_up.shape[1]), BF16), pltpu.VMEM((own_rows, half_cols), BF16),
            pltpu.VMEM((2, rows, half_cols), F32), pltpu.VMEM((rows, half_cols), F32),
            pltpu.VMEM((own_rows, half_cols), F32), pltpu.VMEM((own_rows, half_cols), F32), pltpu.VMEM((own_rows, half_cols), F32),
            pltpu.VMEM((4, own_rows, BLK), F32),
            pltpu.VMEM((2, rows, 3) + heads_f32, F32), pltpu.VMEM((rows, 3) + heads_f32, F32),
            pltpu.VMEM((own_rows,) + heads_f32, F32), pltpu.VMEM((n_far, 2) + heads_f32, F32),
            pltpu.VMEM((own_rows,) + heads_f32, F32), pltpu.VMEM((n_far, 2) + heads_f32, F32),
            dma((6,)), dma, dma, dma((10,)), dma((4,)), dma((n_steps,)), dma((n_steps,)), dma, dma, dma, dma, dma, dma, dma, dma,
            dma((n_all,)), dma((n_all,)), dma((n_far,)), dma((n_far,)), dma((n_far,)), dma((n_far,)), dma((4,)), dma((4,)),
        ],
        compiler_params=pltpu.CompilerParams(collective_id=0, has_side_effects=True, vmem_limit_bytes=27 << 20),
    )(positions, positions.reshape(1, -1), hidden, ln_gamma.reshape(1, -1), ln_beta.reshape(1, -1), cos_full, sin_full,
      w_qkv, w_up, w_down, w_out, k_cache, v_cache)

    z_far = lax.ppermute(z, 'sp', [(0, 2), (2, 0), (1, 3), (3, 1)])

    k_next, v_next = pl.pallas_call(
        store_kernel,
        in_specs=[VM],
        out_specs=[HB, HB],
        out_shape=[jax.ShapeDtypeStruct(k_cache.shape, BF16), jax.ShapeDtypeStruct(k_cache.shape, BF16)],
        scratch_shapes=[pltpu.VMEM((2, rows, HEAD_DIM), F32), pltpu.VMEM((2, rows, 16, HEAD_DIM), BF16),
                        pltpu.VMEM((32, rows), jnp.int32), pltpu.SMEM((32, rows), jnp.int32),
                        dma((2, 8)), dma((2,)), dma],
        compiler_params=pltpu.CompilerParams(vmem_limit_bytes=4 << 20),
        cost_estimate=pl.CostEstimate(flops=40_000_000_000, bytes_accessed=32 << 20, transcendentals=0),
    )(kv)

    branches = jnp.concatenate([jnp.where(upper, z, z_far), jnp.where(upper, z_far, z)], axis=0)
    out_hidden = (hidden.astype(F32) + branches).astype(BF16)
    return out_hidden, k_next, v_next


def solution(mesh):
    cache_spec = P('dp', 'sp', None)
    in_specs = (P('dp', None), P(None), P(None), P(None, None), P(None, None), P(None, 'sp'), P('sp', None), cache_spec, cache_spec, P('dp'))
    out_specs = (P('dp', None), cache_spec, cache_spec)
    return jax.shard_map(device_step, mesh=mesh, in_specs=in_specs, out_specs=out_specs, check_vma=False)
```

```python
import jax
import jax.numpy as jnp
import numpy as np
from jax import lax
from jax.experimental import pallas as pl
from jax.experimental.pallas import tpu as pltpu
from jax.sharding import PartitionSpec as P


MESH = pl.DeviceIdType.MESH
LN_EPS = 1e-5
ROPE_BASE = 10000.0
NEG_FILL = -1e30
HEAD_DIM = 128
BLK = 512
STEP_ROWS = 8
LOOP_ROWS = 16
SKEW = 4
SLOTS = 7
FAR_GROUPS = (32, 32)
OWN_GROUPS = (32, 16, 16)
F32, BF16 = jnp.float32, jnp.bfloat16


def rope_tables(positions):
    inv_freq = (ROPE_BASE ** (-np.arange(0, HEAD_DIM, 2) / HEAD_DIM)).astype(np.float32)
    angles = positions.astype(F32)[:, None] * inv_freq[None, :]
    cos_half, sin_half = jnp.cos(angles), jnp.sin(angles)
    return jnp.concatenate([cos_half, cos_half], axis=-1), jnp.concatenate([-sin_half, sin_half], axis=-1)


def layer_kernel(pos_hbm, posv_hbm, x_hbm, gamma_hbm, beta_hbm, cos_hbm, sin_hbm, wqkv_hbm, wup_hbm, wdown_hbm, wout_hbm,
                 k_hbm, v_hbm, kv_ref, z_ref,
                 pos_ref, posv_ref, gamma_ref, beta_ref, cos_ref, sin_ref,
                 xbuf, hbuf, kvw, wbuf, q_s, kn_ref, vn_ref, act, ctx_ref, part, mrecv, mx_recv, mlp_own, mlp_mate, arecv,
                 s_loc, s_recv, chip_o, chip_ml, x_o, x_ml,
                 insem, xsem, kvwsem, wsem, osem, ksem, vsem, q_ss, q_rs, m_ss, m_rs, mx_ss, mx_rs, mm_ss, mm_rs,
                 c_ss, c_rs, o_ss, o_rs, t_ss, t_rs, a_ss, a_rs):
    dp, sp = lax.axis_index('dp'), lax.axis_index('sp')
    core = lax.rem(sp, 2)
    chip = lax.div(sp, 2)
    mate = (dp, sp + 1 - 2 * core)
    across = (dp, lax.rem(sp + 2, 4))
    rows = xbuf.shape[0]
    own_rows = rows // 2
    n_steps = rows // STEP_ROWS
    seq_dev = k_hbm.shape[1]
    half_heads = q_s.shape[2]
    half_cols = half_heads * HEAD_DIM
    scale = HEAD_DIM ** -0.5
    own_base = pl.multiple_of(chip * own_rows, own_rows)
    far_base = pl.multiple_of((1 - chip) * own_rows, own_rows)

    def weight_copy(src, col, slot, idx):
        return pltpu.make_async_copy(src.at[:, pl.ds(pl.multiple_of(col, BLK), BLK)], wbuf.at[slot], wsem.at[idx])

    def q_copy(j):
        return weight_copy(wqkv_hbm, core * half_cols + j * BLK, j, j)

    def up_copy(j):
        return weight_copy(wup_hbm, j * BLK, 2 + j, 2 + j)

    def down_copy(j):
        half = jnp.where(j < 2, 1 - core, core)
        return weight_copy(wdown_hbm, half * half_cols + lax.rem(j, 2) * BLK, lax.rem(6 + j, SLOTS), 6 + j)

    def out_copy(j):
        half = (1 - core) if j < 2 else core
        src = wout_hbm.at[pl.ds(pl.multiple_of(core * half_cols, half_cols), half_cols),
                          pl.ds(pl.multiple_of(half * half_cols + (j % 2) * BLK, BLK), BLK)]
        return pltpu.make_async_copy(src, wbuf.at[3 + j // 2, pl.ds((j % 2) * half_cols, half_cols)], osem.at[j])

    def first_row(i):
        return pl.multiple_of(lax.rem((1 - chip) * own_rows + i * STEP_ROWS, rows), STEP_ROWS)

    def k_copy(i):
        r = pl.ds(first_row(i), STEP_ROWS)
        return pltpu.make_async_copy(k_hbm.at[r], kv_ref.at[0, r], ksem.at[i])

    def v_copy(i):
        r = pl.ds(first_row(i), STEP_ROWS)
        return pltpu.make_async_copy(v_hbm.at[r], kv_ref.at[1, r], vsem.at[i])

    def cache_start(i):
        k_copy(i).start()
        v_copy(i).start()

    x_copy = pltpu.make_async_copy(x_hbm, xbuf, xsem)
    x_copy.start()
    small = [pltpu.make_async_copy(src, dst, insem.at[n]) for n, (src, dst) in enumerate((
        (gamma_hbm, gamma_ref), (beta_hbm, beta_ref), (cos_hbm, cos_ref), (sin_hbm, sin_ref), (posv_hbm, posv_ref),
        (pos_hbm, pos_ref)))]
    for copy in small:
        copy.start()
    kvw_copy = pltpu.make_async_copy(wqkv_hbm.at[:, pl.ds(2 * half_cols, 2 * HEAD_DIM)], kvw, kvwsem)
    kvw_copy.start()
    for j in range(2):
        q_copy(j).start()
    for j in range(4):
        up_copy(j).start()
    down_copy(0).start()

    barrier = pltpu.get_barrier_semaphore()
    for dev in (mate, across):
        pl.semaphore_signal(barrier, inc=1, device_id=dev, device_id_type=MESH)
    pl.semaphore_wait(barrier, 2)

    x_copy.wait()
    for copy in small:
        copy.wait()

    def norm_rows(i, _):
        for u in range(2):
            r = pl.ds(pl.multiple_of(i * 32 + u * 16, 16), 16)
            h = xbuf[r, :].astype(F32)
            centered = h - jnp.mean(h, axis=-1, keepdims=True)
            var = jnp.mean(centered * centered, axis=-1, keepdims=True)
            hbuf[r, :] = (centered * lax.rsqrt(var + LN_EPS) * gamma_ref[...] + beta_ref[...]).astype(BF16)
        return 0

    lax.fori_loop(0, rows // 32, norm_rows, 0)

    def rotate(vec):
        vec = vec.astype(BF16).astype(F32)
        return (vec * cos_ref[...] + pltpu.roll(vec, HEAD_DIM // 2, 1) * sin_ref[...]).astype(BF16)

    kvw_copy.wait()
    kv_new = jnp.dot(hbuf[...], kvw[...], preferred_element_type=F32)
    k_new = rotate(kv_new[:, :HEAD_DIM])
    v_new = kv_new[:, HEAD_DIM:].astype(BF16)
    kn_ref[...] = k_new.astype(F32)
    vn_ref[...] = v_new.astype(F32)
    kv_ref[0, rows, 0:rows, :] = k_new
    kv_ref[1, rows, 0:rows, :] = v_new
    at = jnp.broadcast_to(posv_ref[...] - sp * seq_dev, (16, rows))
    tile = lax.shift_right_logical(jnp.clip(at, 0, seq_dev - 1), 4)
    inside = jnp.logical_and(at >= 0, at < seq_dev)
    kv_ref[0, rows, rows:rows + 16, :] = tile.astype(F32).astype(BF16)
    kv_ref[0, rows, rows + 16:rows + 32, :] = jnp.where(inside, at - tile * 16, 16).astype(F32).astype(BF16)

    for j in range(2):
        q_copy(j).wait()
        for n in range(2):
            q_part = jnp.dot(hbuf[...], wbuf[j, :, n * 256:(n + 1) * 256], preferred_element_type=F32)
            for t in range(2):
                q_s[core, :, j * 4 + n * 2 + t, :] = rotate(q_part[:, t * HEAD_DIM:(t + 1) * HEAD_DIM]).astype(F32)
        down_copy(1 + j).start()
    q_send = pltpu.make_async_remote_copy(src_ref=q_s.at[core], dst_ref=q_s.at[core], send_sem=q_ss, recv_sem=q_rs,
                                          device_id=mate, device_id_type=MESH)
    q_send.start()

    def up_step(j, _):
        up_copy(j).wait()
        for n in range(2):
            up = jnp.dot(hbuf[...], wbuf[2 + j, :, n * 256:(n + 1) * 256], preferred_element_type=F32)
            gelu = 0.5 * up * (1.0 + lax.erf(up * (0.5 ** 0.5)))
            act[:, pl.ds(pl.multiple_of(j * BLK + n * 256, 256), 256)] = gelu.astype(BF16)

        @pl.when(j == 0)
        def _():
            down_copy(3).start()
            cache_start(0)

        @pl.when(j > 0)
        def _():
            cache_start(2 * j - 1)
            cache_start(2 * j)

        return 0

    lax.fori_loop(0, 4, up_step, 0)

    def down_step(j, _):
        down_copy(j).wait()
        slot = lax.rem(6 + j, SLOTS)
        for n in range(2):
            part[j // 2, :, pl.ds(pl.multiple_of(lax.rem(j, 2) * BLK + n * 256, 256), 256)] = jnp.dot(
                act[...], wbuf[slot, :, n * 256:(n + 1) * 256], preferred_element_type=F32)
        cache_start(7 + 2 * j)
        cache_start(8 + 2 * j)
        return 0

    m_send = pltpu.make_async_remote_copy(src_ref=part.at[0], dst_ref=mrecv, send_sem=m_ss, recv_sem=m_rs,
                                          device_id=mate, device_id_type=MESH)
    lax.fori_loop(0, 2, down_step, 0)
    m_send.start()
    lax.fori_loop(2, 4, down_step, 0)
    cache_start(n_steps - 1)
    for j in range(4):
        out_copy(j).start()
    m_send.wait()
    part[1] = part[1] + mrecv[...]
    mx_send = pltpu.make_async_remote_copy(src_ref=part.at[1, pl.ds(far_base, own_rows)], dst_ref=mx_recv, send_sem=mx_ss,
                                           recv_sem=mx_rs, device_id=across, device_id_type=MESH)
    mx_send.start()
    q_send.wait()

    slots = lax.broadcasted_iota(jnp.int32, (2 * half_heads, seq_dev), 1)
    lanes = lax.broadcasted_iota(jnp.int32, (half_heads, 128), 1)
    zero_q = jnp.zeros((2 * half_heads, HEAD_DIM), BF16)

    def scores(b0):
        bs = [b0, b0 + 1]
        qf = [jnp.concatenate([q_s[0, b], q_s[1, b]], axis=0) for b in bs]
        qb = [q.astype(BF16) for q in qf]
        lhs = jnp.concatenate([jnp.concatenate([qb[0], zero_q], axis=1), jnp.concatenate([zero_q, qb[1]], axis=1)], axis=0)
        k2 = jnp.concatenate([kv_ref[0, b] for b in bs], axis=1)
        return qf, lax.dot_general(lhs, k2, (((1,), (1,)), ((), ())), preferred_element_type=F32)

    def weigh(b0, turn, qf, s2):
        probs, stats = [], []
        for t in range(2):
            b = b0 + t
            at = pos_ref[b] - sp * seq_dev
            s = s2[t * 2 * half_heads:(t + 1) * 2 * half_heads] * scale
            old = slots < at
            here = jnp.logical_and(at >= 0, at < seq_dev)
            masked = jnp.where(old, s, NEG_FILL)
            s_new = jnp.sum(qf[t] * kn_ref[pl.ds(b, 1), :], axis=-1, keepdims=True) * scale
            s_new = jnp.where(here, s_new, NEG_FILL)
            m = jnp.maximum(jnp.max(masked, axis=-1, keepdims=True), s_new)
            e = jnp.where(old, jnp.exp(masked - m), 0.0)
            e_new = jnp.where(here, jnp.exp(s_new - m), 0.0)
            l = jnp.sum(e, axis=-1, keepdims=True) + e_new
            probs.append(e.astype(BF16))
            stats.append((m, l, e_new.astype(BF16).astype(F32) * vn_ref[pl.ds(b, 1), :]))
        v2 = jnp.concatenate([kv_ref[1, b0 + t] for t in range(2)], axis=1)
        o2 = jnp.dot(jnp.concatenate(probs, axis=0), v2, preferred_element_type=F32)
        for t in range(2):
            m, l, extra = stats[t]
            o = o2[t * 2 * half_heads:(t + 1) * 2 * half_heads, t * HEAD_DIM:(t + 1) * HEAD_DIM] + extra
            mb = jnp.broadcast_to(m, o.shape)
            lb = jnp.broadcast_to(l, o.shape)
            for f in range(2):
                hs = slice(f * half_heads, (f + 1) * half_heads)
                s_loc[f, turn + t, 0] = o[hs]
                s_loc[f, turn + t, 1] = mb[hs]
                s_loc[f, turn + t, 2] = lb[hs]

    def attend(i, _):
        per = LOOP_ROWS // STEP_ROWS
        for c in range(per):
            k_copy(i * per + c).wait()
            v_copy(i * per + c).wait()
        row = first_row(i * per)
        pairs = LOOP_ROWS // 2
        ready = {}
        for n in range(pairs + SKEW):
            if n < pairs:
                ready[n] = scores(row + 2 * n)
            if n >= SKEW:
                weigh(row + 2 * (n - SKEW), i * LOOP_ROWS + 2 * (n - SKEW), *ready.pop(n - SKEW))
        return 0

    sizes = FAR_GROUPS + OWN_GROUPS
    starts = [sum(sizes[:g]) for g in range(len(sizes))]
    n_far = len(FAR_GROUPS)

    def swap_copy(g):
        r = pl.ds(starts[g], sizes[g])
        return pltpu.make_async_remote_copy(src_ref=s_loc.at[1 - core, r], dst_ref=s_recv.at[r], send_sem=c_ss.at[g],
                                            recv_sem=c_rs.at[g], device_id=mate, device_id_type=MESH)

    def cross_copies(g):
        r = pl.ds(starts[g], sizes[g])
        return (pltpu.make_async_remote_copy(src_ref=chip_o.at[r], dst_ref=x_o.at[r], send_sem=o_ss.at[g],
                                             recv_sem=o_rs.at[g], device_id=across, device_id_type=MESH),
                pltpu.make_async_remote_copy(src_ref=chip_ml.at[g], dst_ref=x_ml.at[g], send_sem=t_ss.at[g],
                                             recv_sem=t_rs.at[g], device_id=across, device_id_type=MESH))

    def merge_far(g):
        swap_copy(g).wait()

        def body(i, tiles):
            tm, tl = tiles
            for u in range(8):
                b = starts[g] + i * 8 + u
                m_a, m_b = s_loc[core, b, 1], s_recv[b, 1]
                top = jnp.maximum(m_a, m_b)
                w_a, w_b = jnp.exp(m_a - top), jnp.exp(m_b - top)
                chip_o[b] = s_loc[core, b, 0] * w_a + s_recv[b, 0] * w_b
                total = s_loc[core, b, 2] * w_a + s_recv[b, 2] * w_b
                hit = lanes == i * 8 + u
                tm = jnp.where(hit, top, tm)
                tl = jnp.where(hit, total, tl)
            return tm, tl

        zero = jnp.zeros((half_heads, 128), F32)
        tm, tl = lax.fori_loop(0, sizes[g] // 8, body, (zero, zero))
        chip_ml[g, 0] = tm
        chip_ml[g, 1] = tl
        for copy in cross_copies(g):
            copy.start()

    def merge_own(g):
        swap_copy(g).wait()

        def body(i, _):
            for u in range(8):
                b = starts[g] + i * 8 + u
                src = b - own_rows
                part_g = starts[g] - own_rows
                xg = [n for n in range(n_far) if starts[n] <= part_g][-1]
                hit = lanes == src - starts[xg]
                m_x = jnp.sum(jnp.where(hit, x_ml[xg, 0], 0.0), axis=-1, keepdims=True)
                l_x = jnp.sum(jnp.where(hit, x_ml[xg, 1], 0.0), axis=-1, keepdims=True)
                m_a, m_b = s_loc[core, b, 1], s_recv[b, 1]
                top = jnp.maximum(jnp.maximum(m_a, m_b), m_x)
                w_a, w_b, w_x = jnp.exp(m_a - top), jnp.exp(m_b - top), jnp.exp(m_x - top)
                total = s_loc[core, b, 2] * w_a + s_recv[b, 2] * w_b + l_x * w_x
                x_o[src] = (s_loc[core, b, 0] * w_a + s_recv[b, 0] * w_b + x_o[src] * w_x) / total
            return 0

        lax.fori_loop(0, sizes[g] // 8, body, 0)

    def run_group(g):
        lax.fori_loop(starts[g] // LOOP_ROWS, (starts[g] + sizes[g]) // LOOP_ROWS, attend, 0)
        swap_copy(g).start()

    def cross_wait(g):
        for copy in cross_copies(g):
            copy.wait()

    mm_send = pltpu.make_async_remote_copy(src_ref=mlp_own, dst_ref=mlp_mate, send_sem=mm_ss, recv_sem=mm_rs,
                                           device_id=mate, device_id_type=MESH)
    run_group(0)
    run_group(1)
    merge_far(0)
    run_group(2)
    merge_far(1)
    run_group(3)
    mx_send.wait()
    mlp_own[...] = part[1, pl.ds(own_base, own_rows), :] + mx_recv[...]
    mm_send.start()
    run_group(4)
    cross_wait(0)
    merge_own(2)
    cross_wait(1)
    merge_own(3)
    merge_own(4)
    for h in range(half_heads):
        ctx_ref[:, h * HEAD_DIM:(h + 1) * HEAD_DIM] = x_o[:, h, :].astype(BF16)
    mm_send.wait()

    def attn_copy(j):
        return pltpu.make_async_remote_copy(src_ref=part.at[0, pl.ds(j % 2 * own_rows, own_rows), pl.ds(j // 2 * BLK, BLK)],
                                            dst_ref=arecv.at[j], send_sem=a_ss.at[j], recv_sem=a_rs.at[j],
                                            device_id=mate, device_id_type=MESH)

    def block(j):
        return part.at[0, pl.ds(j % 2 * own_rows, own_rows), pl.ds(j // 2 * BLK, BLK)]

    for j in range(4):
        out_copy(j).wait()
        for n in range(2):
            block(j)[:, n * 256:(n + 1) * 256] = jnp.dot(
                ctx_ref[...], wbuf[3 + j // 2, (j % 2) * half_cols:(j % 2 + 1) * half_cols, n * 256:(n + 1) * 256],
                preferred_element_type=F32)
        attn_copy(j).start()
    for j in range(4):
        attn_copy(j).wait()
    for j in range(4):
        half = (1 - core) if j < 2 else core
        mlp = mlp_mate if j < 2 else mlp_own
        col = pl.multiple_of(half * half_cols + (j % 2) * BLK, BLK)
        z_ref[:, pl.ds(col, BLK)] = block(j)[...] + arecv[(j + 2) % 4] + mlp[:, (j % 2) * BLK:(j % 2 + 1) * BLK]


def store_kernel(kv_ref, k_out, v_out, fresh, tiles, idx_v, idx_s, kvsem, tsem, isem):
    rows = k_out.shape[0]
    n_parts = kvsem.shape[1]
    per = rows // n_parts
    outs = (k_out, v_out)

    def big(a, p):
        r = pl.ds(p * per, per)
        return pltpu.make_async_copy(kv_ref.at[a, r], outs[a].at[r], kvsem.at[a, p])

    idx_v[...] = kv_ref[0, rows, rows:rows + 32, :].astype(F32).astype(jnp.int32)
    idx_copy = pltpu.make_async_copy(idx_v, idx_s, isem)
    idx_copy.start()
    for p in range(n_parts):
        for a in range(2):
            big(a, p).start()
    for a in range(2):
        fresh[a] = kv_ref[a, rows, 0:rows, :].astype(F32)
    idx_copy.wait()
    ids = lax.broadcasted_iota(jnp.int32, (16, HEAD_DIM), 0)

    def tile_of(b):
        return pl.ds(pl.multiple_of(idx_s[0, b] * 16, 16), 16)

    def make_tile(b, _):
        hit = ids == idx_s[16, b]
        for a in range(2):
            old = kv_ref[a, b, tile_of(b), :].astype(F32)
            tiles[a, b] = jnp.where(hit, fresh[a, pl.ds(b, 1), :], old).astype(BF16)
        return 0

    lax.fori_loop(0, rows, make_tile, 0, unroll=8)

    for p in range(n_parts):
        for a in range(2):
            big(a, p).wait()

        def put(b, _):
            for a in range(2):
                pltpu.make_async_copy(tiles.at[a, b], outs[a].at[b, tile_of(b)], tsem.at[a]).start()
            return 0

        lax.fori_loop(p * per, (p + 1) * per, put, 0, unroll=4)
    for a in range(2):
        pltpu.make_async_copy(tiles.at[a], outs[a].at[:, pl.ds(0, 16)], tsem.at[a]).wait()


ANY = pl.BlockSpec(memory_space=pl.ANY)
VM = pl.BlockSpec(memory_space=pltpu.VMEM)
SM = pl.BlockSpec(memory_space=pltpu.SMEM)
HB = pl.BlockSpec(memory_space=pltpu.HBM)


def device_step(hidden, ln_gamma, ln_beta, w_qkv, w_out, w_up, w_down, k_cache, v_cache, positions):
    rows, d_model = hidden.shape
    half_heads = w_out.shape[0] // HEAD_DIM // 2
    half_cols = half_heads * HEAD_DIM
    own_rows = rows // 2
    n_steps, n_far, n_all = rows // STEP_ROWS, len(FAR_GROUPS), len(FAR_GROUPS) + len(OWN_GROUPS)
    positions, upper = lax.optimization_barrier((positions, lax.axis_index('sp') < 2))
    cos_full, sin_full = rope_tables(positions)
    dma = pltpu.SemaphoreType.DMA
    heads_f32 = (half_heads, HEAD_DIM)
    kv, z = pl.pallas_call(
        layer_kernel,
        in_specs=[HB] * 13,
        out_specs=[VM] * 2,
        out_shape=[pltpu.VMEM((2, rows + 1) + k_cache.shape[1:], BF16), jax.ShapeDtypeStruct((own_rows, d_model), F32)],
        scratch_shapes=[
            pltpu.SMEM((rows,), jnp.int32), pltpu.VMEM((1, rows), jnp.int32),
            pltpu.VMEM((1, d_model), F32), pltpu.VMEM((1, d_model), F32),
            pltpu.VMEM((rows, HEAD_DIM), F32), pltpu.VMEM((rows, HEAD_DIM), F32),
            pltpu.VMEM((rows, d_model), BF16), pltpu.VMEM((rows, d_model), BF16),
            pltpu.VMEM((d_model, 2 * HEAD_DIM), BF16), pltpu.VMEM((SLOTS, d_model, BLK), BF16),
            pltpu.VMEM((2, rows) + heads_f32, F32),
            pltpu.VMEM((rows, HEAD_DIM), F32), pltpu.VMEM((rows, HEAD_DIM), F32),
            pltpu.VMEM((rows, w_up.shape[1]), BF16), pltpu.VMEM((own_rows, half_cols), BF16),
            pltpu.VMEM((2, rows, half_cols), F32), pltpu.VMEM((rows, half_cols), F32),
            pltpu.VMEM((own_rows, half_cols), F32), pltpu.VMEM((own_rows, half_cols), F32), pltpu.VMEM((own_rows, half_cols), F32),
            pltpu.VMEM((4, own_rows, BLK), F32),
            pltpu.VMEM((2, rows, 3) + heads_f32, F32), pltpu.VMEM((rows, 3) + heads_f32, F32),
            pltpu.VMEM((own_rows,) + heads_f32, F32), pltpu.VMEM((n_far, 2) + heads_f32, F32),
            pltpu.VMEM((own_rows,) + heads_f32, F32), pltpu.VMEM((n_far, 2) + heads_f32, F32),
            dma((6,)), dma, dma, dma((10,)), dma((4,)), dma((n_steps,)), dma((n_steps,)), dma, dma, dma, dma, dma, dma, dma, dma,
            dma((n_all,)), dma((n_all,)), dma((n_far,)), dma((n_far,)), dma((n_far,)), dma((n_far,)), dma((4,)), dma((4,)),
        ],
        compiler_params=pltpu.CompilerParams(collective_id=0, has_side_effects=True, vmem_limit_bytes=29 << 20),
    )(positions, positions.reshape(1, -1), hidden, ln_gamma.reshape(1, -1), ln_beta.reshape(1, -1), cos_full, sin_full,
      w_qkv, w_up, w_down, w_out, k_cache, v_cache)

    z_far = lax.ppermute(z, 'sp', [(0, 2), (2, 0), (1, 3), (3, 1)])

    k_next, v_next = pl.pallas_call(
        store_kernel,
        in_specs=[VM],
        out_specs=[HB, HB],
        out_shape=[jax.ShapeDtypeStruct(k_cache.shape, BF16), jax.ShapeDtypeStruct(k_cache.shape, BF16)],
        scratch_shapes=[pltpu.VMEM((2, rows, HEAD_DIM), F32), pltpu.VMEM((2, rows, 16, HEAD_DIM), BF16),
                        pltpu.VMEM((32, rows), jnp.int32), pltpu.SMEM((32, rows), jnp.int32),
                        dma((2, 8)), dma((2,)), dma],
        compiler_params=pltpu.CompilerParams(vmem_limit_bytes=4 << 20),
        cost_estimate=pl.CostEstimate(flops=40_000_000_000, bytes_accessed=32 << 20, transcendentals=0),
    )(kv)

    branches = jnp.concatenate([jnp.where(upper, z, z_far), jnp.where(upper, z_far, z)], axis=0)
    out_hidden = (hidden.astype(F32) + branches).astype(BF16)
    return out_hidden, k_next, v_next


def solution(mesh):
    cache_spec = P('dp', 'sp', None)
    in_specs = (P('dp', None), P(None), P(None), P(None, None), P(None, None), P(None, 'sp'), P('sp', None), cache_spec, cache_spec, P('dp'))
    out_specs = (P('dp', None), cache_spec, cache_spec)
    return jax.shard_map(device_step, mesh=mesh, in_specs=in_specs, out_specs=out_specs, check_vma=False)
```

```python
import jax
import jax.numpy as jnp
import numpy as np
from jax import lax
from jax.experimental import pallas as pl
from jax.experimental.pallas import tpu as pltpu
from jax.sharding import PartitionSpec as P


MESH = pl.DeviceIdType.MESH
LN_EPS = 1e-5
ROPE_BASE = 10000.0
NEG_FILL = -1e30
HEAD_DIM = 128
BLK = 512
STEP_ROWS = 8
LOOP_ROWS = 16
SKEW = 4
SLOTS = 7
FAR_GROUPS = (16, 16, 16, 16)
OWN_GROUPS = (32, 16, 16)
F32, BF16 = jnp.float32, jnp.bfloat16


def rope_rates():
    inv_freq = (ROPE_BASE ** (-np.arange(0, HEAD_DIM, 2) / HEAD_DIM)).astype(np.float32)
    return np.concatenate([inv_freq, inv_freq])[None, :]


def layer_kernel(pos_hbm, posv_hbm, x_hbm, gamma_hbm, beta_hbm, rate_hbm, wqkv_hbm, wup_hbm, wdown_hbm, wout_hbm,
                 k_hbm, v_hbm, kv_ref, z_ref,
                 pos_ref, posv_ref, gamma_ref, beta_ref, rate_ref, cos_ref, sin_ref,
                 xbuf, hbuf, kvw, wbuf, q_s, kn_ref, vn_ref, act, ctx_ref, part, mrecv, mx_recv, mlp_own, mlp_mate, arecv,
                 s_loc, s_recv, chip_o, chip_ml, x_o, x_ml,
                 insem, xsem, kvwsem, wsem, osem, ksem, vsem, q_ss, q_rs, m_ss, m_rs, mx_ss, mx_rs, mm_ss, mm_rs,
                 c_ss, c_rs, o_ss, o_rs, t_ss, t_rs, a_ss, a_rs):
    dp, sp = lax.axis_index('dp'), lax.axis_index('sp')
    core = lax.rem(sp, 2)
    chip = lax.div(sp, 2)
    mate = (dp, sp + 1 - 2 * core)
    across = (dp, lax.rem(sp + 2, 4))
    rows = xbuf.shape[0]
    own_rows = rows // 2
    seq_dev = k_hbm.shape[1]
    half_heads = q_s.shape[2]
    half_cols = half_heads * HEAD_DIM
    scale = HEAD_DIM ** -0.5
    own_base = pl.multiple_of(chip * own_rows, own_rows)
    far_base = pl.multiple_of((1 - chip) * own_rows, own_rows)

    def weight_copy(src, col, slot, idx):
        return pltpu.make_async_copy(src.at[:, pl.ds(pl.multiple_of(col, BLK), BLK)], wbuf.at[slot], wsem.at[idx])

    def q_copy(j):
        return weight_copy(wqkv_hbm, core * half_cols + j * BLK, 1 + j, 8 + j)

    def up_copy(j):
        return weight_copy(wup_hbm, j * BLK, j, j)

    def down_copy(j):
        half = jnp.where(j < 2, 1 - core, core)
        return weight_copy(wdown_hbm, half * half_cols + lax.rem(j, 2) * BLK, lax.rem(4 + j, SLOTS), 4 + j)

    def out_copy(j):
        half = (1 - core) if j < 2 else core
        src = wout_hbm.at[pl.ds(pl.multiple_of(core * half_cols, half_cols), half_cols),
                          pl.ds(pl.multiple_of(half * half_cols + (j % 2) * BLK, BLK), BLK)]
        return pltpu.make_async_copy(src, wbuf.at[3 + j // 2, pl.ds((j % 2) * half_cols, half_cols)], osem.at[j])

    def first_row(i):
        return pl.multiple_of(lax.rem((1 - chip) * own_rows + i * STEP_ROWS, rows), STEP_ROWS)

    def k_copy(i):
        r = pl.ds(first_row(i), STEP_ROWS)
        return pltpu.make_async_copy(k_hbm.at[r], kv_ref.at[0, r], ksem.at[i])

    def v_copy(i):
        r = pl.ds(first_row(i), STEP_ROWS)
        return pltpu.make_async_copy(v_hbm.at[r], kv_ref.at[1, r], vsem.at[i])

    def cache_start(i):
        k_copy(i).start()
        v_copy(i).start()

    x_copy = pltpu.make_async_copy(x_hbm, xbuf, xsem)
    x_copy.start()
    small = [pltpu.make_async_copy(src, dst, insem.at[n]) for n, (src, dst) in enumerate((
        (gamma_hbm, gamma_ref), (beta_hbm, beta_ref), (rate_hbm, rate_ref), (posv_hbm, posv_ref),
        (pos_hbm, pos_ref)))]
    for copy in small:
        copy.start()
    for j in range(4):
        up_copy(j).start()
    for j in range(3):
        down_copy(j).start()
    kvw_copy = pltpu.make_async_copy(wqkv_hbm.at[:, pl.ds(2 * half_cols, 2 * HEAD_DIM)], kvw, kvwsem)
    kvw_copy.start()

    barrier = pltpu.get_barrier_semaphore()
    for dev in (mate, across):
        pl.semaphore_signal(barrier, inc=1, device_id=dev, device_id_type=MESH)
    pl.semaphore_wait(barrier, 2)

    x_copy.wait()
    for copy in small:
        copy.wait()

    def norm_rows(i, _):
        for u in range(2):
            r = pl.ds(pl.multiple_of(i * 32 + u * 16, 16), 16)
            h = xbuf[r, :].astype(F32)
            centered = h - jnp.mean(h, axis=-1, keepdims=True)
            var = jnp.mean(centered * centered, axis=-1, keepdims=True)
            hbuf[r, :] = (centered * lax.rsqrt(var + LN_EPS) * gamma_ref[...] + beta_ref[...]).astype(BF16)
        return 0

    lax.fori_loop(0, rows // 32, norm_rows, 0)

    turns = jnp.broadcast_to(posv_ref[...], (HEAD_DIM, rows)).astype(F32).T * rate_ref[...]
    lane = lax.broadcasted_iota(jnp.int32, (rows, HEAD_DIM), 1)
    cos_ref[...] = jnp.cos(turns)
    sin_ref[...] = jnp.where(lane < HEAD_DIM // 2, -jnp.sin(turns), jnp.sin(turns))

    def rotate(vec):
        vec = vec.astype(BF16).astype(F32)
        return (vec * cos_ref[...] + pltpu.roll(vec, HEAD_DIM // 2, 1) * sin_ref[...]).astype(BF16)

    def up_step(j, _):
        up_copy(j).wait()
        for n in range(2):
            up = jnp.dot(hbuf[...], wbuf[j, :, n * 256:(n + 1) * 256], preferred_element_type=F32)
            gelu = 0.5 * up * (1.0 + lax.erf(up * (0.5 ** 0.5)))
            act[:, pl.ds(pl.multiple_of(j * BLK + n * 256, 256), 256)] = gelu.astype(BF16)

        @pl.when(j == 0)
        def _():
            down_copy(3).start()

        @pl.when(j == 1)
        def _():
            q_copy(0).start()

        @pl.when(j == 2)
        def _():
            q_copy(1).start()

        @pl.when(j == 3)
        def _():
            cache_start(0)
            cache_start(1)

        return 0

    lax.fori_loop(0, 4, up_step, 0)

    def down_step(j, _):
        down_copy(j).wait()
        slot = lax.rem(4 + j, SLOTS)
        for n in range(2):
            part[j // 2, :, pl.ds(pl.multiple_of(lax.rem(j, 2) * BLK + n * 256, 256), 256)] = jnp.dot(
                act[...], wbuf[slot, :, n * 256:(n + 1) * 256], preferred_element_type=F32)
        cache_start(2 + 2 * j)
        cache_start(3 + 2 * j)
        return 0

    m_send = pltpu.make_async_remote_copy(src_ref=part.at[0], dst_ref=mrecv, send_sem=m_ss, recv_sem=m_rs,
                                          device_id=mate, device_id_type=MESH)
    lax.fori_loop(0, 2, down_step, 0)
    m_send.start()
    lax.fori_loop(2, 4, down_step, 0)
    for j in range(4):
        out_copy(j).start()
    kvw_copy.wait()
    kv_new = jnp.dot(hbuf[...], kvw[...], preferred_element_type=F32)
    k_new = rotate(kv_new[:, :HEAD_DIM])
    v_new = kv_new[:, HEAD_DIM:].astype(BF16)
    kn_ref[...] = k_new.astype(F32)
    vn_ref[...] = v_new.astype(F32)
    kv_ref[0, rows, 0:rows, :] = k_new
    kv_ref[1, rows, 0:rows, :] = v_new
    at = jnp.broadcast_to(posv_ref[...] - sp * seq_dev, (16, rows))
    tile = lax.shift_right_logical(jnp.clip(at, 0, seq_dev - 1), 4)
    inside = jnp.logical_and(at >= 0, at < seq_dev)
    kv_ref[0, rows, rows:rows + 16, :] = tile.astype(F32).astype(BF16)
    kv_ref[0, rows, rows + 16:rows + 32, :] = jnp.where(inside, at - tile * 16, 16).astype(F32).astype(BF16)

    m_send.wait()
    part[1] = part[1] + mrecv[...]
    mx_send = pltpu.make_async_remote_copy(src_ref=part.at[1, pl.ds(far_base, own_rows)], dst_ref=mx_recv, send_sem=mx_ss,
                                           recv_sem=mx_rs, device_id=across, device_id_type=MESH)
    mx_send.start()
    for j in range(2):
        q_copy(j).wait()
        for n in range(2):
            q_part = jnp.dot(hbuf[...], wbuf[1 + j, :, n * 256:(n + 1) * 256], preferred_element_type=F32)
            for t in range(2):
                q_s[core, :, j * 4 + n * 2 + t, :] = rotate(q_part[:, t * HEAD_DIM:(t + 1) * HEAD_DIM]).astype(F32)
        for c in range(3):
            cache_start(10 + 3 * j + c)
    q_send = pltpu.make_async_remote_copy(src_ref=q_s.at[core], dst_ref=q_s.at[core], send_sem=q_ss, recv_sem=q_rs,
                                          device_id=mate, device_id_type=MESH)
    q_send.start()

    q_send.wait()

    slots = lax.broadcasted_iota(jnp.int32, (2 * half_heads, seq_dev), 1)
    lanes = lax.broadcasted_iota(jnp.int32, (half_heads, 128), 1)
    zero_q = jnp.zeros((2 * half_heads, HEAD_DIM), BF16)

    def scores(b0):
        bs = [b0, b0 + 1]
        qf = [jnp.concatenate([q_s[0, b], q_s[1, b]], axis=0) for b in bs]
        qb = [q.astype(BF16) for q in qf]
        lhs = jnp.concatenate([jnp.concatenate([qb[0], zero_q], axis=1), jnp.concatenate([zero_q, qb[1]], axis=1)], axis=0)
        k2 = jnp.concatenate([kv_ref[0, b] for b in bs], axis=1)
        return qf, lax.dot_general(lhs, k2, (((1,), (1,)), ((), ())), preferred_element_type=F32)

    def weigh(b0, turn, qf, s2):
        probs, stats = [], []
        for t in range(2):
            b = b0 + t
            at = pos_ref[b] - sp * seq_dev
            s = s2[t * 2 * half_heads:(t + 1) * 2 * half_heads] * scale
            old = slots < at
            here = jnp.logical_and(at >= 0, at < seq_dev)
            masked = jnp.where(old, s, NEG_FILL)
            s_new = jnp.sum(qf[t] * kn_ref[pl.ds(b, 1), :], axis=-1, keepdims=True) * scale
            s_new = jnp.where(here, s_new, NEG_FILL)
            m = jnp.maximum(jnp.max(masked, axis=-1, keepdims=True), s_new)
            e = jnp.where(old, jnp.exp(masked - m), 0.0)
            e_new = jnp.where(here, jnp.exp(s_new - m), 0.0)
            l = jnp.sum(e, axis=-1, keepdims=True) + e_new
            probs.append(e.astype(BF16))
            stats.append((m, l, e_new.astype(BF16).astype(F32) * vn_ref[pl.ds(b, 1), :]))
        v2 = jnp.concatenate([kv_ref[1, b0 + t] for t in range(2)], axis=1)
        o2 = jnp.dot(jnp.concatenate(probs, axis=0), v2, preferred_element_type=F32)
        for t in range(2):
            m, l, extra = stats[t]
            o = o2[t * 2 * half_heads:(t + 1) * 2 * half_heads, t * HEAD_DIM:(t + 1) * HEAD_DIM] + extra
            mb = jnp.broadcast_to(m, o.shape)
            lb = jnp.broadcast_to(l, o.shape)
            for f in range(2):
                hs = slice(f * half_heads, (f + 1) * half_heads)
                s_loc[f, turn + t, 0] = o[hs]
                s_loc[f, turn + t, 1] = mb[hs]
                s_loc[f, turn + t, 2] = lb[hs]

    def attend(i, _):
        per = LOOP_ROWS // STEP_ROWS
        for c in range(per):
            k_copy(i * per + c).wait()
            v_copy(i * per + c).wait()
        row = first_row(i * per)
        pairs = LOOP_ROWS // 2
        ready = {}
        for n in range(pairs + SKEW):
            if n < pairs:
                ready[n] = scores(row + 2 * n)
            if n >= SKEW:
                weigh(row + 2 * (n - SKEW), i * LOOP_ROWS + 2 * (n - SKEW), *ready.pop(n - SKEW))
        return 0

    sizes = FAR_GROUPS + OWN_GROUPS
    starts = [sum(sizes[:g]) for g in range(len(sizes))]
    n_far = len(FAR_GROUPS)

    def swap_copy(g):
        r = pl.ds(starts[g], sizes[g])
        return pltpu.make_async_remote_copy(src_ref=s_loc.at[1 - core, r], dst_ref=s_recv.at[r], send_sem=c_ss.at[g],
                                            recv_sem=c_rs.at[g], device_id=mate, device_id_type=MESH)

    def cross_copies(g):
        r = pl.ds(starts[g], sizes[g])
        return (pltpu.make_async_remote_copy(src_ref=chip_o.at[r], dst_ref=x_o.at[r], send_sem=o_ss.at[g],
                                             recv_sem=o_rs.at[g], device_id=across, device_id_type=MESH),
                pltpu.make_async_remote_copy(src_ref=chip_ml.at[g], dst_ref=x_ml.at[g], send_sem=t_ss.at[g],
                                             recv_sem=t_rs.at[g], device_id=across, device_id_type=MESH))

    def merge_far(g):
        swap_copy(g).wait()

        def body(i, tiles):
            tm, tl = tiles
            for u in range(8):
                b = starts[g] + i * 8 + u
                m_a, m_b = s_loc[core, b, 1], s_recv[b, 1]
                top = jnp.maximum(m_a, m_b)
                w_a, w_b = jnp.exp(m_a - top), jnp.exp(m_b - top)
                chip_o[b] = s_loc[core, b, 0] * w_a + s_recv[b, 0] * w_b
                total = s_loc[core, b, 2] * w_a + s_recv[b, 2] * w_b
                hit = lanes == i * 8 + u
                tm = jnp.where(hit, top, tm)
                tl = jnp.where(hit, total, tl)
            return tm, tl

        zero = jnp.zeros((half_heads, 128), F32)
        tm, tl = lax.fori_loop(0, sizes[g] // 8, body, (zero, zero))
        chip_ml[g, 0] = tm
        chip_ml[g, 1] = tl
        for copy in cross_copies(g):
            copy.start()

    def merge_own(g):
        swap_copy(g).wait()

        def body(i, _):
            for u in range(8):
                b = starts[g] + i * 8 + u
                src = b - own_rows
                xg = lax.div(src, FAR_GROUPS[0])
                hit = lanes == lax.rem(src, FAR_GROUPS[0])
                m_x = jnp.sum(jnp.where(hit, x_ml[xg, 0], 0.0), axis=-1, keepdims=True)
                l_x = jnp.sum(jnp.where(hit, x_ml[xg, 1], 0.0), axis=-1, keepdims=True)
                m_a, m_b = s_loc[core, b, 1], s_recv[b, 1]
                top = jnp.maximum(jnp.maximum(m_a, m_b), m_x)
                w_a, w_b, w_x = jnp.exp(m_a - top), jnp.exp(m_b - top), jnp.exp(m_x - top)
                total = s_loc[core, b, 2] * w_a + s_recv[b, 2] * w_b + l_x * w_x
                x_o[src] = (s_loc[core, b, 0] * w_a + s_recv[b, 0] * w_b + x_o[src] * w_x) / total
            return 0

        lax.fori_loop(0, sizes[g] // 8, body, 0)

    def run_group(g):
        lax.fori_loop(starts[g] // LOOP_ROWS, (starts[g] + sizes[g]) // LOOP_ROWS, attend, 0)
        swap_copy(g).start()

    def cross_wait(g):
        for copy in cross_copies(g):
            copy.wait()

    mm_send = pltpu.make_async_remote_copy(src_ref=mlp_own, dst_ref=mlp_mate, send_sem=mm_ss, recv_sem=mm_rs,
                                           device_id=mate, device_id_type=MESH)
    for g in range(n_far + 1):
        run_group(g)
        if g > 0:
            merge_far(g - 1)
    run_group(n_far + 1)
    mx_send.wait()
    mlp_own[...] = part[1, pl.ds(own_base, own_rows), :] + mx_recv[...]
    mm_send.start()
    run_group(n_far + 2)
    for g in range(n_far):
        cross_wait(g)
    for g in range(n_far, len(sizes)):
        merge_own(g)
    for h in range(half_heads):
        ctx_ref[:, h * HEAD_DIM:(h + 1) * HEAD_DIM] = x_o[:, h, :].astype(BF16)
    mm_send.wait()

    def attn_copy(j):
        return pltpu.make_async_remote_copy(src_ref=part.at[0, pl.ds(j % 2 * own_rows, own_rows), pl.ds(j // 2 * BLK, BLK)],
                                            dst_ref=arecv.at[j], send_sem=a_ss.at[j], recv_sem=a_rs.at[j],
                                            device_id=mate, device_id_type=MESH)

    def block(j):
        return part.at[0, pl.ds(j % 2 * own_rows, own_rows), pl.ds(j // 2 * BLK, BLK)]

    for j in range(4):
        out_copy(j).wait()
        for n in range(2):
            block(j)[:, n * 256:(n + 1) * 256] = jnp.dot(
                ctx_ref[...], wbuf[3 + j // 2, (j % 2) * half_cols:(j % 2 + 1) * half_cols, n * 256:(n + 1) * 256],
                preferred_element_type=F32)
        attn_copy(j).start()
    for j in range(4):
        attn_copy(j).wait()
    for j in range(4):
        half = (1 - core) if j < 2 else core
        mlp = mlp_mate if j < 2 else mlp_own
        col = pl.multiple_of(half * half_cols + (j % 2) * BLK, BLK)
        z_ref[:, pl.ds(col, BLK)] = block(j)[...] + arecv[(j + 2) % 4] + mlp[:, (j % 2) * BLK:(j % 2 + 1) * BLK]


def store_kernel(kv_ref, k_out, v_out, fresh, tiles, idx_v, idx_s, kvsem, tsem, isem):
    rows = k_out.shape[0]
    n_parts = kvsem.shape[1]
    per = rows // n_parts
    outs = (k_out, v_out)

    def big(a, p):
        r = pl.ds(p * per, per)
        return pltpu.make_async_copy(kv_ref.at[a, r], outs[a].at[r], kvsem.at[a, p])

    idx_v[...] = kv_ref[0, rows, rows:rows + 32, :].astype(F32).astype(jnp.int32)
    idx_copy = pltpu.make_async_copy(idx_v, idx_s, isem)
    idx_copy.start()
    for p in range(n_parts):
        for a in range(2):
            big(a, p).start()
    for a in range(2):
        fresh[a] = kv_ref[a, rows, 0:rows, :].astype(F32)
    idx_copy.wait()
    ids = lax.broadcasted_iota(jnp.int32, (16, HEAD_DIM), 0)

    def tile_of(b):
        return pl.ds(pl.multiple_of(idx_s[0, b] * 16, 16), 16)

    def make_tile(b, _):
        hit = ids == idx_s[16, b]
        for a in range(2):
            old = kv_ref[a, b, tile_of(b), :].astype(F32)
            tiles[a, b] = jnp.where(hit, fresh[a, pl.ds(b, 1), :], old).astype(BF16)
        return 0

    lax.fori_loop(0, rows, make_tile, 0, unroll=8)

    for p in range(n_parts):
        for a in range(2):
            big(a, p).wait()

        def put(b, _):
            for a in range(2):
                pltpu.make_async_copy(tiles.at[a, b], outs[a].at[b, tile_of(b)], tsem.at[a]).start()
            return 0

        lax.fori_loop(p * per, (p + 1) * per, put, 0, unroll=4)
    for a in range(2):
        pltpu.make_async_copy(tiles.at[a], outs[a].at[:, pl.ds(0, 16)], tsem.at[a]).wait()


ANY = pl.BlockSpec(memory_space=pl.ANY)
VM = pl.BlockSpec(memory_space=pltpu.VMEM)
SM = pl.BlockSpec(memory_space=pltpu.SMEM)
HB = pl.BlockSpec(memory_space=pltpu.HBM)


def device_step(hidden, ln_gamma, ln_beta, w_qkv, w_out, w_up, w_down, k_cache, v_cache, positions):
    rows, d_model = hidden.shape
    half_heads = w_out.shape[0] // HEAD_DIM // 2
    half_cols = half_heads * HEAD_DIM
    own_rows = rows // 2
    n_steps, n_far, n_all = rows // STEP_ROWS, len(FAR_GROUPS), len(FAR_GROUPS) + len(OWN_GROUPS)
    positions, upper = lax.optimization_barrier((positions, lax.axis_index('sp') < 2))
    dma = pltpu.SemaphoreType.DMA
    heads_f32 = (half_heads, HEAD_DIM)
    kv, z = pl.pallas_call(
        layer_kernel,
        in_specs=[HB] * 12,
        out_specs=[VM] * 2,
        out_shape=[pltpu.VMEM((2, rows + 1) + k_cache.shape[1:], BF16), jax.ShapeDtypeStruct((own_rows, d_model), F32)],
        scratch_shapes=[
            pltpu.SMEM((rows,), jnp.int32), pltpu.VMEM((1, rows), jnp.int32),
            pltpu.VMEM((1, d_model), F32), pltpu.VMEM((1, d_model), F32), pltpu.VMEM((1, HEAD_DIM), F32),
            pltpu.VMEM((rows, HEAD_DIM), F32), pltpu.VMEM((rows, HEAD_DIM), F32),
            pltpu.VMEM((rows, d_model), BF16), pltpu.VMEM((rows, d_model), BF16),
            pltpu.VMEM((d_model, 2 * HEAD_DIM), BF16), pltpu.VMEM((SLOTS, d_model, BLK), BF16),
            pltpu.VMEM((2, rows) + heads_f32, F32),
            pltpu.VMEM((rows, HEAD_DIM), F32), pltpu.VMEM((rows, HEAD_DIM), F32),
            pltpu.VMEM((rows, w_up.shape[1]), BF16), pltpu.VMEM((own_rows, half_cols), BF16),
            pltpu.VMEM((2, rows, half_cols), F32), pltpu.VMEM((rows, half_cols), F32),
            pltpu.VMEM((own_rows, half_cols), F32), pltpu.VMEM((own_rows, half_cols), F32), pltpu.VMEM((own_rows, half_cols), F32),
            pltpu.VMEM((4, own_rows, BLK), F32),
            pltpu.VMEM((2, rows, 3) + heads_f32, F32), pltpu.VMEM((rows, 3) + heads_f32, F32),
            pltpu.VMEM((own_rows,) + heads_f32, F32), pltpu.VMEM((n_far, 2) + heads_f32, F32),
            pltpu.VMEM((own_rows,) + heads_f32, F32), pltpu.VMEM((n_far, 2) + heads_f32, F32),
            dma((5,)), dma, dma, dma((10,)), dma((4,)), dma((n_steps,)), dma((n_steps,)), dma, dma, dma, dma, dma, dma, dma, dma,
            dma((n_all,)), dma((n_all,)), dma((n_far,)), dma((n_far,)), dma((n_far,)), dma((n_far,)), dma((4,)), dma((4,)),
        ],
        compiler_params=pltpu.CompilerParams(collective_id=0, has_side_effects=True, vmem_limit_bytes=29 << 20),
    )(positions, positions.reshape(1, -1), hidden, ln_gamma.reshape(1, -1), ln_beta.reshape(1, -1), rope_rates(),
      w_qkv, w_up, w_down, w_out, k_cache, v_cache)

    z_far = lax.ppermute(z, 'sp', [(0, 2), (2, 0), (1, 3), (3, 1)])

    k_next, v_next = pl.pallas_call(
        store_kernel,
        in_specs=[VM],
        out_specs=[HB, HB],
        out_shape=[jax.ShapeDtypeStruct(k_cache.shape, BF16), jax.ShapeDtypeStruct(k_cache.shape, BF16)],
        scratch_shapes=[pltpu.VMEM((2, rows, HEAD_DIM), F32), pltpu.VMEM((2, rows, 16, HEAD_DIM), BF16),
                        pltpu.VMEM((32, rows), jnp.int32), pltpu.SMEM((32, rows), jnp.int32),
                        dma((2, 8)), dma((2,)), dma],
        compiler_params=pltpu.CompilerParams(vmem_limit_bytes=4 << 20),
        cost_estimate=pl.CostEstimate(flops=40_000_000_000, bytes_accessed=32 << 20, transcendentals=0),
    )(kv)

    branches = jnp.concatenate([jnp.where(upper, z, z_far), jnp.where(upper, z_far, z)], axis=0)
    out_hidden = (hidden.astype(F32) + branches).astype(BF16)
    return out_hidden, k_next, v_next


def solution(mesh):
    cache_spec = P('dp', 'sp', None)
    in_specs = (P('dp', None), P(None), P(None), P(None, None), P(None, None), P(None, 'sp'), P('sp', None), cache_spec, cache_spec, P('dp'))
    out_specs = (P('dp', None), cache_spec, cache_spec)
    return jax.shard_map(device_step, mesh=mesh, in_specs=in_specs, out_specs=out_specs, check_vma=False)
```
